32 devices in a mesh: dp: 8 (over z, core), tensor: 4 (over y, x).
Axes of the slice: x: 2, y: 2, z: 4, core: 2. Of those that a mesh axis runs over, the one named last changes fastest.
Arguments:
- streams: bfloat16 [4, 20480, 2048], P(None, ('dp', 'tensor')), may hold values from -6 to 6
- prior: bfloat16 [3, 20480, 2048], P(None, ('dp', 'tensor')), may hold values from -6 to 6
- seg_ids: int32 [20480], P('dp'), may hold values from 0 to 2, as said below
- positions: int32 [20480], P('dp'), may hold values from 0 to 2558, as said below
- w_qk: bfloat16 [2, 2048, 2048], P(None, 'dp', 'tensor'), may hold values from -0.1875 to 0.1875
- w_value: bfloat16 [2048, 2048], P('dp', 'tensor'), may hold values from -0.125 to 0.125
- w_out: bfloat16 [2048, 2048], P('tensor', 'dp'), may hold values from -0.5 to 0.5
- w_up: bfloat16 [2048, 8192], P('dp', 'tensor'), may hold values from -0.125 to 0.125
- w_down: bfloat16 [8192, 2048], P('tensor', 'dp'), may hold values from -0.0625 to 0.0625
- norm_gain: bfloat16 [5, 2048], P(None, 'dp'), may hold values from 0.099609375 to 1.8984375
- norm_bias: bfloat16 [5, 2048], P(None, 'dp'), may hold values from -3 to 3
- mix_in: bfloat16 [2048, 16], P('dp'), may hold values from -0.125 to 0.125
- mix_out: bfloat16 [16, 16], P(None, 'dp'), may hold values from -1.5 to 1.5
- mix_bias: bfloat16 [16], P('dp'), may hold values from -3 to 3
- d_streams: bfloat16 [4, 20480, 2048], P(None, ('dp', 'tensor')), may hold values from -6 to 6
Outputs:
- new_streams: bfloat16 [4, 20480, 2048], P(None, ('dp', 'tensor'))
- grad_streams: bfloat16 [4, 20480, 2048], P(None, ('dp', 'tensor'))
- grad_prior: bfloat16 [3, 20480, 2048], P(None, ('dp', 'tensor'))
- grad_w_qk: float32 [2, 2048, 2048], P(None, 'dp', 'tensor')
- grad_w_value: float32 [2048, 2048], P('dp', 'tensor')
- grad_w_out: float32 [2048, 2048], P('tensor', 'dp')
- grad_w_up: float32 [2048, 8192], P('dp', 'tensor')
- grad_w_down: float32 [8192, 2048], P('tensor', 'dp')
- grad_norm_gain: float32 [5, 2048], P(None, 'dp')
- grad_norm_bias: float32 [5, 2048], P(None, 'dp')
- grad_mix_in: float32 [2048, 16], P('dp')
- grad_mix_out: float32 [16, 16], P(None, 'dp')
- grad_mix_bias: float32 [16], P('dp')
The draws below stay inside these ranges and needn't reach their ends.
Inputs may be any that keep to these rules, and one draw needn't show every extreme that they name: `seg_ids`: each group of 2560 consecutive tokens holds 2048 prompt tokens of segment 0 followed by 2 continuations of 256 tokens; every token of a continuation carries that continuation's segment, a number of 1 to 2; several continuations of a group may carry the same segment, and the first continuation of every group carries 2. Prompt tokens have positions 0 to 2047 in order; a continuation's positions rise by one from a start between 2048 and 2303, and the first continuation of every group starts at the latest.
All inputs are finite; a program needn't handle non-finite values.
Results may differ from the reference program's by a relative error of at most 0.02.
Values may be sent and summed in bfloat16 or wider, within the bound.
A program may use at most 512 MiB of HBM per device.

```python
import math
import jax
import jax.numpy as jnp
from jax import lax

D = 2048
HEADS = 16
HDIM = 128
FF = 8192
PRIOR = 3
MIXW = 16
MIXH = 16
PROMPT = 2048
CLEN = 256
CONT = 2
GROUP_TOK = 2560
TOKENS = 20480


def layout(seed_key):
    groups = TOKENS // GROUP_TOK
    labels = jax.random.randint(jax.random.fold_in(seed_key, 101), (groups, CONT), 1, CONT + 1).astype(jnp.int32)
    first_column = jnp.arange(CONT, dtype=jnp.int32)[None, :] == 0
    labels = jnp.where(first_column, CONT, labels).astype(jnp.int32)
    offsets = jax.random.randint(jax.random.fold_in(seed_key, 202), (groups, CONT), 0, CLEN).astype(jnp.int32)
    offsets = jnp.where(first_column, CLEN - 1, offsets).astype(jnp.int32)
    prompt_segments = jnp.zeros((groups, PROMPT), jnp.int32)
    segments = jnp.concatenate([prompt_segments, jnp.repeat(labels, CLEN, axis=1)], axis=1).reshape(-1)
    steps_inside = jnp.tile(jnp.arange(CLEN, dtype=jnp.int32), CONT)[None, :]
    later_positions = PROMPT + jnp.repeat(offsets, CLEN, axis=1) + steps_inside
    prompt_positions = jnp.broadcast_to(jnp.arange(PROMPT, dtype=jnp.int32)[None, :], (groups, PROMPT))
    position_rows = jnp.concatenate([prompt_positions, later_positions.astype(jnp.int32)], axis=1).reshape(-1)
    return (segments, position_rows)


def draw_seg_ids(key, part):
    return layout(key)[0]


def draw_positions(key, part):
    return layout(key)[1]


def level_of(stream_key, extent, shards, smallest, top_value):
    level = 1.0
    for position, blocks in shards:
        heights = jax.random.uniform(jax.random.fold_in(jax.random.fold_in(stream_key, 6), position), (blocks,), jnp.float32, smallest / len(shards), top_value / len(shards))
        level = level * jnp.repeat(jnp.exp(heights), extent[position] // blocks).reshape((-1,) + (1,) * (len(extent) - 1 - position))
    return level


def centred(stream_key, dims, deviation, most, shards=(), held_as=jnp.bfloat16):
    values = deviation * jax.random.normal(stream_key, dims, jnp.float32)
    if shards:
        values = values * level_of(stream_key, dims, shards, -0.22, 0.18)
    return jnp.clip(values, -most, most).astype(held_as)


def setup_inputs(seed: int = 0) -> dict:
    arg_keys = jax.random.split(jax.random.key(seed), 16)
    return {
        "streams": centred(arg_keys[0], (4, TOKENS, D), 1.0, 6.0, ((1, 32),)),
        "prior": centred(arg_keys[1], (PRIOR, TOKENS, D), 1.0, 6.0, ((1, 32),)),
        "seg_ids": draw_seg_ids(jax.random.fold_in(arg_keys[15], 71), 0),
        "positions": draw_positions(jax.random.fold_in(arg_keys[15], 71), 0),
        "w_qk": centred(arg_keys[4], (2, D, D), (D // 2) ** -0.5, 0.1875, ((1, 8), (2, 4))),
        "w_value": centred(arg_keys[5], (D, D), D ** -0.5, 0.125, ((0, 8), (1, 4))),
        "w_out": centred(arg_keys[6], (D, D), (D // 16) ** -0.5, 0.5, ((0, 4), (1, 8))),
        "w_up": centred(arg_keys[7], (D, FF), D ** -0.5, 0.125, ((0, 8), (1, 4))),
        "w_down": centred(arg_keys[8], (FF, D), FF ** -0.5, 0.0625, ((0, 4), (1, 8))),
        "norm_gain": jnp.clip(1.0 + 0.18 * jax.random.normal(arg_keys[9], (5, D), jnp.float32), 0.099609375, 1.8984375).astype(jnp.bfloat16),
        "norm_bias": centred(arg_keys[10], (5, D), 0.5, 3.0, ((1, 8),)),
        "mix_in": centred(arg_keys[11], (D, MIXH), D ** -0.5, 0.125, ((0, 8),)),
        "mix_out": centred(arg_keys[12], (MIXH, MIXW), MIXH ** -0.5, 1.5, ((1, 8),)),
        "mix_bias": centred(arg_keys[13], (MIXW,), 0.5, 3.0, ((0, 8),)),
        "d_streams": centred(arg_keys[14], (4, TOKENS, D), 1.0, 6.0, ((1, 32),)),
    }


@jax.custom_vjp
def low(v):
    return lax.optimization_barrier(v.astype(jnp.bfloat16)).astype(jnp.float32)

@jax.custom_vjp
def low_back(v):
    return v

def low_keep(v):
    return (low(v), None)

def low_pass(kept, grad):
    return (grad,)

def back_keep(v):
    return (v, None)

def back_low(kept, grad):
    return (low(grad),)
low.defvjp(low_keep, low_pass)
low_back.defvjp(back_keep, back_low)
EPSILON = 1e-05
MASKED_SCORE = -1e+30
HIGHEST_PRECISION = lax.Precision.HIGHEST

def layer_norm(inputs, gain_row, shift_row):
    centre = inputs - lax.optimization_barrier(jnp.mean(inputs, axis=-1, keepdims=True))
    spread = lax.optimization_barrier(jnp.mean(centre * centre, axis=-1, keepdims=True))
    return centre * lax.rsqrt(spread + EPSILON) * gain_row + shift_row

def rotary_tables(position_row, head_width):
    half_width = head_width // 2
    frequency = jnp.exp(jnp.arange(half_width, dtype=jnp.float32) * (-2.0 * math.log(10000.0) / head_width))
    angles = position_row.astype(jnp.float32)[:, None] * frequency[None, :]
    return (jnp.cos(angles)[:, None, :], jnp.sin(angles)[:, None, :])

def rotate(inputs, cosine_table, sine_table):
    half_width = inputs.shape[-1] // 2
    first_half = inputs[..., :half_width]
    second_half = inputs[..., half_width:]
    return jnp.concatenate([first_half * cosine_table - second_half * sine_table, second_half * cosine_table + first_half * sine_table], axis=-1)

def visible(segment_query, position_query, segment_keys, position_keys):
    shared = (segment_keys[None, :] == 0) | (segment_keys[None, :] == segment_query[:, None])
    return shared & (position_keys[None, :] <= position_query[:, None])

def product(left, right):
    return jnp.dot(left, right, preferred_element_type=jnp.float32, precision=HIGHEST_PRECISION)

def group_layer(weights, stream_group, prior_group, segment_row, position_row):
    w_qk, w_value, w_out, w_up, w_down, norm_gain, norm_bias, mix_in, mix_out, mix_bias = weights
    group_rows = stream_group.shape[1]
    normed_q = low(layer_norm(stream_group[0], norm_gain[0], norm_bias[0]))
    normed_k = low(layer_norm(stream_group[1], norm_gain[1], norm_bias[1]))
    normed_v = low(layer_norm(stream_group[2], norm_gain[2], norm_bias[2]))
    cosine_table, sine_table = rotary_tables(position_row, HDIM)
    query_rot = low(rotate(low_back(product(normed_q, w_qk[0])).reshape(group_rows, HEADS, HDIM), cosine_table, sine_table))
    key_rot = low(rotate(low_back(product(normed_k, w_qk[1])).reshape(group_rows, HEADS, HDIM), cosine_table, sine_table))
    value_heads = low(low_back(product(normed_v, w_value))).reshape(group_rows, HEADS, HDIM)
    block_rows = min(512, group_rows)
    block_count = group_rows // block_rows
    score_scale = 1.0 / math.sqrt(HDIM)

    def one_block(block_index):
        first_row = block_index * block_rows
        query_block = lax.dynamic_slice_in_dim(query_rot, first_row, block_rows)
        scores = low_back(jnp.einsum('qhe,khe->hqk', query_block, key_rot, precision=HIGHEST_PRECISION) * score_scale)
        pairs = visible(lax.dynamic_slice_in_dim(segment_row, first_row, block_rows), lax.dynamic_slice_in_dim(position_row, first_row, block_rows), segment_row, position_row)
        block_probs = jax.nn.softmax(jnp.where(pairs[None], scores, MASKED_SCORE), axis=-1)
        return jnp.einsum('hqk,khe->qhe', low(block_probs), value_heads, precision=HIGHEST_PRECISION)
    attended = lax.map(jax.checkpoint(one_block), jnp.arange(block_count, dtype=jnp.int32))
    attended = low(low_back(attended.reshape(group_rows, D)))
    mid_stream = stream_group[3] + low_back(product(attended, w_out))
    mlp_input = low(layer_norm(mid_stream, norm_gain[3], norm_bias[3]))
    hidden = low(jax.nn.gelu(low_back(product(mlp_input, w_up)), approximate=False))
    layer_out = mid_stream + low_back(product(hidden, w_down))
    mix_normed = low(layer_norm(layer_out, norm_gain[4], norm_bias[4]))
    mix_act = jax.nn.gelu(low_back(product(mix_normed, mix_in)), approximate=False)
    mix_coef = (product(mix_act, mix_out) + mix_bias).reshape(group_rows, 4, PRIOR + 1)
    sources = jnp.concatenate([prior_group, layer_out[None]], axis=0)
    return jnp.einsum('rsj,jrd->srd', mix_coef, sources, precision=HIGHEST_PRECISION)

def forward(values, seg_ids, positions):
    streams = values[0]
    prior = values[1]
    weights = values[2:]
    group_count = seg_ids.shape[0] // GROUP_TOK
    stream_groups = streams.reshape(4, group_count, GROUP_TOK, D).transpose(1, 0, 2, 3)
    prior_groups = prior.reshape(PRIOR, group_count, GROUP_TOK, D).transpose(1, 0, 2, 3)
    segment_groups = seg_ids.reshape(group_count, GROUP_TOK)
    position_groups = positions.reshape(group_count, GROUP_TOK)
    layer_step = jax.checkpoint(group_layer)

    def scan_step(running, group_items):
        return (running, layer_step(weights, group_items[0], group_items[1], group_items[2], group_items[3]))
    running, outputs = lax.scan(scan_step, jnp.zeros((), jnp.float32), (stream_groups, prior_groups, segment_groups, position_groups))
    return outputs.transpose(1, 0, 2, 3).reshape(4, group_count * GROUP_TOK, D)

def reference(streams, prior, seg_ids, positions, w_qk, w_value, w_out, w_up, w_down, norm_gain, norm_bias, mix_in, mix_out, mix_bias, d_streams):
    floats = tuple((array.astype(jnp.float32) for array in (streams, prior, w_qk, w_value, w_out, w_up, w_down, norm_gain, norm_bias, mix_in, mix_out, mix_bias)))

    def wrapped(*values):
        return forward(values, seg_ids, positions)
    mixed, pull_back = jax.vjp(wrapped, *floats)
    grads = pull_back(d_streams.astype(jnp.float32))
    return (mixed.astype(jnp.bfloat16), grads[0].astype(jnp.bfloat16), grads[1].astype(jnp.bfloat16), grads[2], grads[3], grads[4], grads[5], grads[6], grads[7], grads[8], grads[9], grads[10], grads[11])
```

```python
import functools
import math

import jax
import jax.numpy as jnp
from jax import lax
from jax.experimental import pallas as pl
from jax.experimental.pallas import tpu as pltpu
from jax.sharding import PartitionSpec as P

HDIM = 128
MASKED_SCORE = -1e30
SCORE_SCALE = 1.0 / math.sqrt(HDIM)
LOG2_SCALE = SCORE_SCALE * math.log2(math.e)

def dot_nt(a, b):
    return lax.dot_general(a, b, (((1,), (1,)), ((), ())), preferred_element_type=jnp.float32)

def dot_nn(a, b):
    return lax.dot_general(a, b, (((1,), (0,)), ((), ())), preferred_element_type=jnp.float32)

def seen(pos_col, seg_col, pos_row, seg_row):
    return ((seg_col == 0) | (seg_col == seg_row)) & (pos_col <= pos_row)

def attend_kernel(block, q_ref, k_ref, v_ref, pc_ref, sc_ref, pr_ref, sr_ref, o_ref, l_ref, vt_ref):
    index = pl.program_id(1)

    @pl.when(index == 0)
    def _():
        vt_ref[...] = v_ref[...].T

    query = q_ref[...]

    def step(first, state, masked):
        top, total, acc = state
        rows = pl.ds(pl.multiple_of(first, block), block)
        scores = dot_nt(k_ref[rows, :], query) * LOG2_SCALE
        if masked:
            pairs = seen(pc_ref[rows, :], sc_ref[rows, :], pr_ref[...], sr_ref[...])
            scores = jnp.where(pairs, scores, MASKED_SCORE)
        new_top = jnp.maximum(top, jnp.max(scores, axis=0, keepdims=True))
        fade = jnp.exp2(top - new_top)
        probs = jnp.exp2(scores - new_top)
        total = total * fade + jnp.sum(probs, axis=0, keepdims=True)
        acc = acc * fade + dot_nn(vt_ref[:, rows], probs.astype(jnp.bfloat16))
        return new_top, total, acc

    state = (
        jnp.full((1, block), MASKED_SCORE, jnp.float32),
        jnp.zeros((1, block), jnp.float32),
        jnp.zeros((HDIM, block), jnp.float32),
    )
    state = lax.fori_loop(0, index, lambda j, s: step(j * block, s, False), state)
    top, total, acc = step(index * block, state, True)
    o_ref[...] = (acc / total).T.astype(jnp.bfloat16)
    l_ref[0] = top + jnp.log2(total)

def attend(q, k, v, pos, seg, block=512):
    rows, cols = q.shape
    heads = cols // HDIM
    grid = (heads, rows // block)
    tile = pl.BlockSpec((block, HDIM), lambda h, i: (i, h))
    whole = pl.BlockSpec((rows, HDIM), lambda h, i: (0, h))
    col = pl.BlockSpec((rows, 1), lambda h, i: (0, 0))
    row = pl.BlockSpec((1, block), lambda h, i: (0, i))
    return pl.pallas_call(
        functools.partial(attend_kernel, block),
        grid=grid,
        in_specs=[tile, whole, whole, col, col, row, row],
        out_specs=[tile, pl.BlockSpec((1, 1, block), lambda h, i: (h, 0, i))],
        out_shape=[
            jax.ShapeDtypeStruct((rows, cols), jnp.bfloat16),
            jax.ShapeDtypeStruct((heads, 1, rows), jnp.float32),
        ],
        scratch_shapes=[pltpu.VMEM((HDIM, rows), jnp.bfloat16)],
        cost_estimate=pl.CostEstimate(flops=30_000_000_000, bytes_accessed=4 * rows * cols * 2, transcendentals=0),
        name="attend",
    )(q, k, v, pos[:, None], seg[:, None], pos[None, :], seg[None, :])

def attend_back_kernel(block, q_ref, k_ref, v_ref, o_ref, go_ref, l_ref, pc_ref, sc_ref, pr_ref, sr_ref,
                       ck_ref, sk_ref, cq_ref, sq_ref, dq_ref, dk_ref, dv_ref, kt_ref, ak_ref, av_ref):
    index = pl.program_id(1)

    @pl.when(index == 0)
    def _():
        kt_ref[...] = k_ref[...].T

    query = q_ref[...]
    grad = go_ref[...]
    delta = jnp.sum((o_ref[...].astype(jnp.float32) * grad.astype(jnp.float32)).T, axis=0, keepdims=True)
    logs = l_ref[0]

    def step(first, acc, masked):
        rows = pl.ds(pl.multiple_of(first, block), block)
        scores = dot_nt(k_ref[rows, :], query) * LOG2_SCALE
        if masked:
            pairs = seen(pc_ref[rows, :], sc_ref[rows, :], pr_ref[...], sr_ref[...])
            scores = jnp.where(pairs, scores, MASKED_SCORE)
        probs = jnp.exp2(scores - logs)
        slopes = dot_nt(v_ref[rows, :], grad)
        turned = (probs * (slopes - delta)).astype(jnp.bfloat16)
        add_k = dot_nn(turned, query)
        add_v = dot_nn(probs.astype(jnp.bfloat16), grad)
        if masked:
            ak_ref[rows, :] = add_k
            av_ref[rows, :] = add_v
        else:
            ak_ref[rows, :] += add_k
            av_ref[rows, :] += add_v
        return acc + dot_nn(kt_ref[:, rows], turned)

    acc = lax.fori_loop(0, index, lambda j, s: step(j * block, s, False), jnp.zeros((HDIM, block), jnp.float32))
    acc = step(index * block, acc, True)

    def unturn(value, cosine, sine):
        value = value * SCORE_SCALE
        return (value * cosine - pltpu.roll(value, HDIM // 2, 1) * sine).astype(jnp.bfloat16)

    dq_ref[...] = unturn(acc.T, cq_ref[...], sq_ref[...])

    @pl.when(index == pl.num_programs(1) - 1)
    def _():
        @pl.loop(0, pl.num_programs(1))
        def _(j):
            rows = pl.ds(pl.multiple_of(j * block, block), block)
            dk_ref[rows, :] = unturn(ak_ref[rows, :], ck_ref[rows, :], sk_ref[rows, :])
            dv_ref[rows, :] = av_ref[rows, :].astype(jnp.bfloat16)

def attend_back(q, k, v, o, go, logs, pos, seg, cos2, sin2, block=512):
    rows, cols = q.shape
    heads = cols // HDIM
    grid = (heads, rows // block)
    tile = pl.BlockSpec((block, HDIM), lambda h, i: (i, h))
    whole = pl.BlockSpec((rows, HDIM), lambda h, i: (0, h))
    col = pl.BlockSpec((rows, 1), lambda h, i: (0, 0))
    row = pl.BlockSpec((1, block), lambda h, i: (0, i))
    table = pl.BlockSpec((rows, HDIM), lambda h, i: (0, 0))
    table_tile = pl.BlockSpec((block, HDIM), lambda h, i: (i, 0))
    like = jax.ShapeDtypeStruct((rows, cols), jnp.bfloat16)
    return pl.pallas_call(
        functools.partial(attend_back_kernel, block),
        grid=grid,
        in_specs=[tile, whole, whole, tile, tile, pl.BlockSpec((1, 1, block), lambda h, i: (h, 0, i)),
                  col, col, row, row, table, table, table_tile, table_tile],
        out_specs=[tile, whole, whole],
        out_shape=[like, like, like],
        scratch_shapes=[pltpu.VMEM((HDIM, rows), jnp.bfloat16), pltpu.VMEM((rows, HDIM), jnp.float32),
                        pltpu.VMEM((rows, HDIM), jnp.float32)],
        cost_estimate=pl.CostEstimate(flops=80_000_000_000, bytes_accessed=8 * rows * cols * 2, transcendentals=0),
        name="attend_back",
    )(q, k, v, o, go, logs, pos[:, None], seg[:, None], pos[None, :], seg[None, :], cos2, sin2, cos2, sin2)

EPSILON = 1e-05
HIGHEST_PRECISION = lax.Precision.HIGHEST
ROOT_HALF = math.sqrt(0.5)
PDF_SCALE = 1.0 / math.sqrt(2.0 * math.pi)

def gelu_pair(u):
    cdf = 0.5 + 0.5 * lax.erf(u * ROOT_HALF)
    return u * cdf, cdf + u * (PDF_SCALE * jnp.exp(-0.5 * u * u))

def exact_dot(a, b, dims):
    return lax.dot_general(a, b, (dims, ((), ())), precision=HIGHEST_PRECISION, preferred_element_type=jnp.float32)

def low_dot(a, b, dims):
    return lax.dot_general(a, b, (dims, ((), ())), preferred_element_type=jnp.float32)

def standard(x):
    width = x.shape[-1]
    centre = x - jnp.sum(x, axis=-1, keepdims=True) * (1.0 / width)
    spread = jnp.sum(centre * centre, axis=-1, keepdims=True) * (1.0 / width)
    rstd = lax.rsqrt(spread + EPSILON)
    return centre * rstd, rstd

def pull_standard(xhat, rstd, w):
    width = xhat.shape[-1]
    mean_w = jnp.sum(w, axis=-1, keepdims=True) * (1.0 / width)
    mean_wx = jnp.sum(w * xhat, axis=-1, keepdims=True) * (1.0 / width)
    return (w - mean_w - xhat * mean_wx) * rstd

def row_tile(rows, most):
    tile = min(most, rows)
    while rows % tile:
        tile -= 16
    return tile

def norm_kernel(x_ref, gain_ref, shift_ref, n_ref):
    xhat, _ = standard(x_ref[0].astype(jnp.float32))
    n_ref[0] = (xhat * gain_ref[0] + shift_ref[0]).astype(jnp.bfloat16)

def norm_streams(x, count, gains, shifts):
    rows, width = x.shape[1:]
    tile = row_tile(rows, 128)
    block = pl.BlockSpec((1, tile, width), lambda s, i: (s, i, 0))
    vec = pl.BlockSpec((1, 1, width), lambda s, i: (s, 0, 0))
    return pl.pallas_call(
        norm_kernel, grid=(count, rows // tile), in_specs=[block, vec, vec], out_specs=block,
        out_shape=jax.ShapeDtypeStruct((count, rows, width), jnp.bfloat16), name="norm_streams",
    )(x, gains[:, None, :], shifts[:, None, :])

def mixer_kernel(mid_ref, part_ref, left_ref, right_ref, prior_ref, up_ref, gain_ref, shift_ref,
                 mixin_ref, mixout_ref, bias_ref,
                 new_ref, gprior_ref, gout_ref, gz_ref, gin_ref, gmo_ref, gmb_ref, gg_ref, gs_ref):
    first = pl.program_id(0) == 0
    sources = prior_ref.shape[0] + 1
    count = up_ref.shape[0]
    tile = mid_ref.shape[0]
    wide = count * sources
    out = mid_ref[...] + part_ref[...].astype(jnp.float32) + left_ref[...].astype(jnp.float32) + right_ref[...].astype(jnp.float32)
    xhat, rstd = standard(out)
    gain = gain_ref[...]
    c = (xhat * gain + shift_ref[...]).astype(jnp.bfloat16)
    g = low_dot(c, mixin_ref[...], ((1,), (1,)))
    act, slope = gelu_pair(g)
    coef = exact_dot(act, mixout_ref[...], ((1,), (0,))) + bias_ref[...]
    x = [prior_ref[j].astype(jnp.float32) for j in range(sources - 1)] + [out]
    u = [up_ref[s].astype(jnp.float32) for s in range(count)]
    co = [[coef[:, s * sources + j : s * sources + j + 1] for j in range(sources)] for s in range(count)]
    lane = lax.broadcasted_iota(jnp.int32, (tile, wide), 1)
    gcoef = jnp.zeros((tile, wide), jnp.float32)
    for s in range(count):
        mixed = co[s][0] * x[0]
        for j in range(1, sources):
            mixed = mixed + co[s][j] * x[j]
        new_ref[s] = mixed.astype(jnp.bfloat16)
        for j in range(sources):
            inner = jnp.sum(u[s] * x[j], axis=-1, keepdims=True)
            gcoef = jnp.where(lane == s * sources + j, inner, gcoef)
    for j in range(sources):
        total = co[0][j] * u[0]
        for s in range(1, count):
            total = total + co[s][j] * u[s]
        if j < sources - 1:
            gprior_ref[j] = total.astype(jnp.bfloat16)
    gact = exact_dot(gcoef, mixout_ref[...], ((1,), (1,)))
    gg = (gact * slope).astype(jnp.bfloat16)
    gc = low_dot(gg, mixin_ref[...], ((1,), (0,)))
    gout = total + pull_standard(xhat, rstd, gc * gain)
    gout_ref[...] = gout
    gz_ref[...] = gout.astype(jnp.bfloat16)

    @pl.when(first)
    def _():
        for ref in (gin_ref, gmo_ref, gmb_ref, gg_ref, gs_ref):
            ref[...] = jnp.zeros_like(ref)

    gin_ref[...] += low_dot(gg, c, ((0,), (0,)))
    gmo_ref[...] += exact_dot(act, gcoef, ((0,), (0,)))
    gmb_ref[...] += jnp.sum(gcoef, axis=0, keepdims=True)
    gg_ref[...] += jnp.sum(gc * xhat, axis=0, keepdims=True)
    gs_ref[...] += jnp.sum(gc, axis=0, keepdims=True)

def mixer(mid, parts, prior, d_streams, gain, shift, mix_in, mix_out, mix_bias, most=64):
    rows, width = mid.shape
    hidden = mix_in.shape[0]
    wide = mix_out.shape[1]
    tile = row_tile(rows, most)
    flat = pl.BlockSpec((tile, width), lambda i: (i, 0))
    stack = lambda n: pl.BlockSpec((n, tile, width), lambda i: (0, i, 0))
    full = lambda *s: pl.BlockSpec(s, lambda i: (0,) * len(s))
    f32 = jnp.float32
    shape = jax.ShapeDtypeStruct
    return pl.pallas_call(
        mixer_kernel, grid=(rows // tile,),
        in_specs=[flat, flat, flat, flat, stack(prior.shape[0]), stack(d_streams.shape[0]),
                  full(1, width), full(1, width), full(hidden, width), full(hidden, wide), full(1, wide)],
        out_specs=[stack(d_streams.shape[0]), stack(prior.shape[0]), flat, flat,
                   full(hidden, width), full(hidden, wide), full(1, wide), full(1, width), full(1, width)],
        out_shape=[shape(d_streams.shape, jnp.bfloat16), shape(prior.shape, jnp.bfloat16),
                   shape((rows, width), f32), shape((rows, width), jnp.bfloat16),
                   shape((hidden, width), f32), shape((hidden, wide), f32), shape((1, wide), f32),
                   shape((1, width), f32), shape((1, width), f32)],
        cost_estimate=pl.CostEstimate(flops=1000000, bytes_accessed=60_000_000, transcendentals=0),
        name="mixer",
    )(mid, *parts, prior, d_streams, gain[None], shift[None], mix_in, mix_out, mix_bias[None])

def middle_kernel(attn_ref, stream_ref, gain_ref, shift_ref, mid_ref, m_ref):
    mid = attn_ref[...] + stream_ref[0].astype(jnp.float32)
    mid_ref[...] = mid
    xhat, _ = standard(mid)
    m_ref[...] = (xhat * gain_ref[...] + shift_ref[...]).astype(jnp.bfloat16)

def middle(attn, streams, gain, shift):
    rows, width = attn.shape
    tile = row_tile(rows, 128)
    flat = pl.BlockSpec((tile, width), lambda i: (i, 0))
    vec = pl.BlockSpec((1, width), lambda i: (0, 0))
    return pl.pallas_call(
        middle_kernel, grid=(rows // tile,),
        in_specs=[flat, pl.BlockSpec((1, tile, width), lambda i: (3, i, 0)), vec, vec],
        out_specs=[flat, flat],
        out_shape=[jax.ShapeDtypeStruct((rows, width), jnp.float32), jax.ShapeDtypeStruct((rows, width), jnp.bfloat16)],
        name="middle",
    )(attn, streams, gain[None], shift[None])

def middle_back(mid, gout, parts, gain):
    rows, width = mid.shape
    tile = row_tile(rows, 64)
    flat = pl.BlockSpec((tile, width), lambda i: (i, 0))
    vec = pl.BlockSpec((1, width), lambda i: (0, 0))
    shape = jax.ShapeDtypeStruct
    return pl.pallas_call(
        middle_back_kernel, grid=(rows // tile,),
        in_specs=[flat] * 5 + [vec], out_specs=[flat, vec, vec],
        out_shape=[shape((rows, width), jnp.bfloat16), shape((1, width), jnp.float32), shape((1, width), jnp.float32)],
        name="middle_back",
    )(mid, gout, *parts, gain[None])

def middle_back_kernel(mid_ref, gout_ref, part_ref, left_ref, right_ref, gain_ref, low_ref, gg_ref, gs_ref):
    xhat, rstd = standard(mid_ref[...])
    r = part_ref[...].astype(jnp.float32) + left_ref[...].astype(jnp.float32) + right_ref[...].astype(jnp.float32)
    low_ref[...] = (gout_ref[...] + pull_standard(xhat, rstd, r * gain_ref[...])).astype(jnp.bfloat16)

    @pl.when(pl.program_id(0) == 0)
    def _():
        gg_ref[...] = jnp.zeros_like(gg_ref)
        gs_ref[...] = jnp.zeros_like(gs_ref)

    gg_ref[...] += jnp.sum(r * xhat, axis=0, keepdims=True)
    gs_ref[...] += jnp.sum(r, axis=0, keepdims=True)

def streams_back_kernel(x_ref, rq_ref, rk_ref, rv_ref, last_ref, gain_ref, gx_ref, gg_ref, gs_ref):
    @pl.when(pl.program_id(0) == 0)
    def _():
        gg_ref[...] = jnp.zeros_like(gg_ref)
        gs_ref[...] = jnp.zeros_like(gs_ref)

    for s, ref in enumerate((rq_ref, rk_ref, rv_ref)):
        xhat, rstd = standard(x_ref[s].astype(jnp.float32))
        r = ref[...]
        gx_ref[s] = pull_standard(xhat, rstd, r * gain_ref[s]).astype(jnp.bfloat16)
        gg_ref[s] += jnp.sum(r * xhat, axis=0, keepdims=True)
        gs_ref[s] += jnp.sum(r, axis=0, keepdims=True)
    gx_ref[3] = last_ref[...]

def streams_back(x, rq, rk, rv, last, gains):
    rows, width = rq.shape
    tile = row_tile(rows, 64)
    flat = pl.BlockSpec((tile, width), lambda i: (i, 0))
    three = pl.BlockSpec((3, 1, width), lambda i: (0, 0, 0))
    shape = jax.ShapeDtypeStruct
    return pl.pallas_call(
        streams_back_kernel, grid=(rows // tile,),
        in_specs=[pl.BlockSpec((3, tile, width), lambda i: (0, i, 0)), flat, flat, flat, flat, three],
        out_specs=[pl.BlockSpec((4, tile, width), lambda i: (0, i, 0)), three, three],
        out_shape=[shape((4, rows, width), jnp.bfloat16), shape((3, 1, width), jnp.float32), shape((3, 1, width), jnp.float32)],
        name="streams_back",
    )(x, rq, rk, rv, last, gains[:, None, :])

def project_kernel(turn, swap, n_ref, w_ref, *rest):
    if turn:
        c_ref, s_ref, o_ref = rest
    else:
        (o_ref,) = rest
    y = low_dot(n_ref[...], w_ref[0], ((1,), (1 if swap else 0,)))
    if turn:
        for h in range(y.shape[1] // 128):
            cols = slice(h * 128, (h + 1) * 128)
            part = y[:, cols]
            o_ref[0, :, cols] = (part * c_ref[...] + pltpu.roll(part, 64, 1) * s_ref[...]).astype(jnp.bfloat16)
    else:
        o_ref[0] = y.astype(jnp.bfloat16)

def project(n, w4, tables=None, swap=False, name="project"):
    rows, width = n.shape
    groups = w4.shape[0]
    cols = w4.shape[1] if swap else w4.shape[2]
    specs = [pl.BlockSpec((rows, width), lambda g: (0, 0)), pl.BlockSpec((1,) + w4.shape[1:], lambda g: (g, 0, 0))]
    args = [n, w4]
    if tables is not None:
        specs += [pl.BlockSpec((rows, 128), lambda g: (0, 0))] * 2
        args += list(tables)
    return pl.pallas_call(
        functools.partial(project_kernel, tables is not None, swap), grid=(groups,),
        in_specs=specs, out_specs=pl.BlockSpec((1, rows, cols), lambda g: (g, 0, 0)),
        out_shape=jax.ShapeDtypeStruct((groups, rows, cols), jnp.bfloat16),
        cost_estimate=pl.CostEstimate(flops=2 * rows * width * cols * groups, bytes_accessed=w4.size * 2, transcendentals=0),
        name=name,
    )(*args)

def join_kernel(swap, a_ref, w_ref, o_ref):
    total = None
    for g in range(a_ref.shape[0]):
        part = low_dot(a_ref[g], w_ref[g], ((1,), (1 if swap else 0,)))
        total = part if total is None else total + part
    o_ref[...] = total

def join(a4, w4, swap=False, name="join"):
    groups, rows, cols = a4.shape
    width = w4.shape[1] if swap else w4.shape[2]
    tile = 512
    if swap:
        spec = pl.BlockSpec((groups, tile, cols), lambda i: (0, i, 0))
    else:
        spec = pl.BlockSpec((groups, cols, tile), lambda i: (0, 0, i))
    return pl.pallas_call(
        functools.partial(join_kernel, swap), grid=(width // tile,),
        in_specs=[pl.BlockSpec((groups, rows, cols), lambda i: (0, 0, 0)), spec],
        out_specs=pl.BlockSpec((rows, tile), lambda i: (0, i)),
        out_shape=jax.ShapeDtypeStruct((rows, width), jnp.float32),
        cost_estimate=pl.CostEstimate(flops=2 * rows * width * cols * groups, bytes_accessed=w4.size * 2, transcendentals=0),
        name=name,
    )(a4, w4)

def weight_kernel(swap, n_ref, a_ref, o_ref, t_ref):
    if swap:
        o_ref[0] = low_dot(a_ref[0].T, n_ref[...], ((1,), (0,))).astype(jnp.bfloat16)
    else:
        @pl.when(pl.program_id(0) == 0)
        def _():
            t_ref[...] = n_ref[...].T
        o_ref[0] = low_dot(t_ref[...], a_ref[0], ((1,), (0,))).astype(jnp.bfloat16)

def weight_grad(n, a4, swap=False, name="weight_grad"):
    rows, width = n.shape
    groups, _, cols = a4.shape
    out = (cols, width) if swap else (width, cols)
    return pl.pallas_call(
        functools.partial(weight_kernel, swap), grid=(groups,),
        in_specs=[pl.BlockSpec((rows, width), lambda g: (0, 0)), pl.BlockSpec((1, rows, cols), lambda g: (g, 0, 0))],
        out_specs=pl.BlockSpec((1,) + out, lambda g: (g, 0, 0)),
        out_shape=jax.ShapeDtypeStruct((groups,) + out, jnp.bfloat16),
        scratch_shapes=[pltpu.VMEM((8, 128) if swap else (width, rows), jnp.bfloat16)],
        cost_estimate=pl.CostEstimate(flops=2 * rows * width * cols * groups, bytes_accessed=groups * width * cols * 2, transcendentals=0),
        name=name,
    )(n, a4)


def rotary_tables(position_row):
    half_width = HDIM // 2
    frequency = jnp.exp(
        jnp.arange(half_width, dtype=jnp.float32) * (-2.0 * math.log(10000.0) / HDIM)
    )
    angles = position_row.astype(jnp.float32)[:, None] * frequency[None, :]
    cosine, sine = jnp.cos(angles), jnp.sin(angles)
    return jnp.concatenate([cosine, cosine], axis=1), jnp.concatenate([-sine, sine], axis=1)


def hop(value, mask):
    size = lax.axis_size("tensor")
    return lax.ppermute(value, "tensor", [(i, i ^ mask) for i in range(size)])


def spread_rows(own):
    if lax.axis_size("tensor") != 4:
        return [lax.all_gather(own, "tensor", axis=0, tiled=True)]
    half = own.shape[0] // 2
    one, two = hop(own, 1), hop(own, 2)
    return [own, one, two, hop(one[:half], 2), hop(two[half:], 1)]


def collect_rows(pieces):
    if lax.axis_size("tensor") != 4:
        total = lax.psum_scatter(pieces[0], "tensor", scatter_dimension=0, tiled=True)
        zero = jnp.zeros_like(total)
        return total, zero, zero
    own, one, two, far_low, far_high = pieces
    half = own.shape[0] // 2
    low = hop(far_low, 1)
    high = hop(far_high, 2)
    f32 = jnp.float32
    two = jnp.concatenate(
        [(two[:half].astype(f32) + low.astype(f32)).astype(jnp.bfloat16), two[half:]]
    )
    one = jnp.concatenate(
        [one[:half], (one[half:].astype(f32) + high.astype(f32)).astype(jnp.bfloat16)]
    )
    return own, hop(one, 1), hop(two, 2)


def sum_tensor(value):
    if lax.axis_size("tensor") != 4:
        return lax.psum(value, "tensor")
    value = value + hop(value, 1)
    return value + hop(value, 2)


def exchange(value):
    return lax.all_to_all(value, "tensor", split_axis=0, concat_axis=0, tiled=True)


def full_weight(shard, axis):
    parts = lax.all_gather(shard, "tensor", axis=0, tiled=False)
    return lax.all_gather(parts, "dp", axis=axis + 1, tiled=True)


def reduce_weight(parts, axis):
    mine = lax.psum_scatter(parts, "dp", scatter_dimension=axis + 1, tiled=True)
    return lax.psum_scatter(mine, "tensor", scatter_dimension=0, tiled=False).astype(jnp.float32)


def contract_first(left, right):
    return low_dot(left, right, ((0,), (0,)))


def contract_last(left, right):
    return low_dot(left, right, ((1,), (1,)))


def split_columns(value):
    size = lax.axis_size("dp")
    rows, cols = value.shape
    return value.reshape(rows, size, cols // size).transpose(1, 0, 2).reshape(size, -1)


def reduce_small(values):
    size = lax.axis_size("dp")
    packed = jnp.concatenate([split_columns(value) for value in values], axis=1)
    length = packed.shape[1]
    rows = -(-length // 1024) * 8
    packed = jnp.pad(packed, ((0, 0), (0, rows * 128 - length))).reshape(size, rows, 128)
    mine = lax.psum_scatter(packed, "dp", scatter_dimension=0, tiled=False)
    mine = sum_tensor(mine).reshape(-1)
    result, first = [], 0
    for value in values:
        count = value.shape[0] * value.shape[1] // size
        result.append(mine[first : first + count].reshape(value.shape[0], -1))
        first += count
    return result


def gather_small(values):
    size = lax.axis_size("dp")
    packed = jnp.concatenate([value.reshape(-1) for value in values])
    length = packed.shape[0]
    rows = -(-length // 2048) * 16
    packed = jnp.pad(packed, (0, rows * 128 - length)).reshape(rows, 128)
    every = lax.all_gather(packed, "dp", axis=0, tiled=False).reshape(size, -1)
    result, first = [], 0
    for value in values:
        count = value.size
        block = every[:, first : first + count].reshape(size, value.shape[0], -1)
        result.append(block.transpose(1, 0, 2).reshape(value.shape[0], -1))
        first += count
    return result


def body(
    streams,
    prior,
    seg_ids,
    positions,
    w_qk,
    w_value,
    w_out,
    w_up,
    w_down,
    norm_gain,
    norm_bias,
    mix_in,
    mix_out,
    mix_bias,
    d_streams,
):
    rows_dev = streams.shape[1]
    bf16 = jnp.bfloat16
    place = lax.axis_index("tensor")
    gains, shifts, mixin_cols, mixout_all, mixbias_all = gather_small(
        [norm_gain, norm_bias, mix_in.T, mix_out, mix_bias[None]]
    )
    gains, shifts = gains.astype(jnp.float32), shifts.astype(jnp.float32)
    mixout_all, mixbias_all = mixout_all.astype(jnp.float32), mixbias_all.astype(jnp.float32)
    query_full = full_weight(w_qk[0], 0)
    key_full = full_weight(w_qk[1], 0)
    value_full = full_weight(w_value, 0)
    out_full = full_weight(w_out, 1)
    up_all = lax.all_gather(w_up, "dp", axis=0, tiled=True)
    down_all = lax.all_gather(w_down, "dp", axis=1, tiled=True)

    tables = rotary_tables(positions)
    own_tables = [lax.dynamic_slice_in_dim(t, place * rows_dev, rows_dev) for t in tables]
    normed = norm_streams(streams, 3, gains[:3], shifts[:3])
    query = exchange(project(normed[0], query_full, own_tables, name="query"))
    key = exchange(project(normed[1], key_full, own_tables, name="key"))
    value = exchange(project(normed[2], value_full, name="value"))
    heads_shape = (value.shape[0] * value.shape[1], value.shape[2])
    query, key, value = (x.reshape(heads_shape) for x in (query, key, value))
    attended, logs = attend(query, key, value, positions, seg_ids)
    attended_rows = exchange(attended.reshape(-1, rows_dev, heads_shape[1]))
    attn_result = join(attended_rows, out_full, name="attn_out")
    mid, mlp_input = middle(attn_result, streams, gains[3], shifts[3])

    mlp_rows = spread_rows(mlp_input)
    hidden, slopes, parts = [], [], []
    for rows in mlp_rows:
        acts, slope = gelu_pair(low_dot(rows, up_all, ((1,), (0,))))
        hidden.append(acts.astype(bf16))
        slopes.append(slope.astype(bf16))
        parts.append(low_dot(hidden[-1], down_all, ((1,), (0,))).astype(bf16))
    parts = collect_rows(parts)
    (
        new_streams,
        grad_prior,
        grad_layer,
        grad_layer_low,
        grad_mix_in,
        grad_mix_out,
        grad_mix_bias,
        gain_four,
        shift_four,
    ) = mixer(
        mid, parts, prior, d_streams, gains[4], shifts[4], mixin_cols, mixout_all, mixbias_all[0]
    )

    grad_rows = spread_rows(grad_layer_low)
    grad_pre, parts = [], []
    for rows, slope in zip(grad_rows, slopes):
        grad_hidden = contract_last(rows, down_all)
        grad_pre.append((grad_hidden * slope.astype(jnp.float32)).astype(bf16))
        parts.append(contract_last(grad_pre[-1], up_all).astype(bf16))
    parts = collect_rows(parts)
    grad_w_down = contract_first(jnp.concatenate(hidden), jnp.concatenate(grad_rows)).astype(bf16)
    grad_w_up = contract_first(jnp.concatenate(mlp_rows), jnp.concatenate(grad_pre)).astype(bf16)
    grad_mid, gain_three, shift_three = middle_back(mid, grad_layer, parts, gains[3])

    grad_attended = exchange(project(grad_mid, out_full, swap=True, name="attn_out_back"))
    grad_query, grad_key, grad_value = attend_back(
        query,
        key,
        value,
        attended,
        grad_attended.reshape(heads_shape),
        logs,
        positions,
        seg_ids,
        *tables,
    )
    grad_w_out = weight_grad(grad_mid, attended_rows, swap=True, name="grad_w_out")
    back, grads = [], []
    for index, (grad, full) in enumerate(
        ((grad_query, query_full), (grad_key, key_full), (grad_value, value_full))
    ):
        rows = exchange(grad.reshape(-1, rows_dev, heads_shape[1]))
        grads.append(weight_grad(normed[index], rows, name="grad_w_in"))
        back.append(join(rows, full, swap=True, name="attn_in_back"))
    grad_streams, gain_first, shift_first = streams_back(streams, *back, grad_mid, gains[:3])

    shard_up = lax.psum_scatter(grad_w_up, "dp", scatter_dimension=0, tiled=True)
    shard_down = lax.psum_scatter(grad_w_down, "dp", scatter_dimension=1, tiled=True)
    shard_out = reduce_weight(grad_w_out, 1)
    shard_query, shard_key, shard_value = (reduce_weight(grad, 0) for grad in grads)
    late_gain, late_shift, total_mix_in, total_mix_out, total_mix_bias = reduce_small(
        [
            jnp.concatenate([gain_three, gain_four]),
            jnp.concatenate([shift_three, shift_four]),
            grad_mix_in,
            grad_mix_out,
            grad_mix_bias,
        ]
    )
    early_gain, early_shift = reduce_small([gain_first[:, 0], shift_first[:, 0]])
    return (
        new_streams,
        grad_streams,
        grad_prior,
        jnp.stack([shard_query, shard_key]),
        shard_value,
        shard_out,
        shard_up.astype(jnp.float32),
        shard_down.astype(jnp.float32),
        jnp.concatenate([early_gain, late_gain]),
        jnp.concatenate([early_shift, late_shift]),
        total_mix_in.T,
        total_mix_out,
        total_mix_bias[0],
    )


def solution(mesh):
    in_specs = (
        P(None, ("dp", "tensor"), None),
        P(None, ("dp", "tensor"), None),
        P("dp"),
        P("dp"),
        P(None, "dp", "tensor"),
        P("dp", "tensor"),
        P("tensor", "dp"),
        P("dp", "tensor"),
        P("tensor", "dp"),
        P(None, "dp"),
        P(None, "dp"),
        P("dp", None),
        P(None, "dp"),
        P("dp"),
        P(None, ("dp", "tensor"), None),
    )
    out_specs = (
        P(None, ("dp", "tensor"), None),
        P(None, ("dp", "tensor"), None),
        P(None, ("dp", "tensor"), None),
        P(None, "dp", "tensor"),
        P("dp", "tensor"),
        P("tensor", "dp"),
        P("dp", "tensor"),
        P("tensor", "dp"),
        P(None, "dp"),
        P(None, "dp"),
        P("dp", None),
        P(None, "dp"),
        P("dp"),
    )
    return jax.shard_map(body, mesh=mesh, in_specs=in_specs, out_specs=out_specs, check_vma=False)
```

```python
import functools
import math

import jax
import jax.numpy as jnp
from jax import lax
from jax.experimental import pallas as pl
from jax.experimental.pallas import tpu as pltpu
from jax.sharding import PartitionSpec as P

HDIM = 128
MASKED_SCORE = -1e30
SCORE_SCALE = 1.0 / math.sqrt(HDIM)
LOG2_SCALE = SCORE_SCALE * math.log2(math.e)

def dot_nt(a, b):
    return lax.dot_general(a, b, (((1,), (1,)), ((), ())), preferred_element_type=jnp.float32)

def dot_nn(a, b):
    return lax.dot_general(a, b, (((1,), (0,)), ((), ())), preferred_element_type=jnp.float32)

def seen(pos_col, seg_col, pos_row, seg_row):
    return ((seg_col == 0) | (seg_col == seg_row)) & (pos_col <= pos_row)

def attend_kernel(block, q_ref, k_ref, v_ref, pc_ref, sc_ref, pr_ref, sr_ref, o_ref, l_ref, vt_ref):
    index = pl.program_id(1)

    @pl.when(index == 0)
    def _():
        vt_ref[...] = v_ref[...].T

    query = q_ref[...]

    def step(first, state, masked):
        top, total, acc = state
        rows = pl.ds(pl.multiple_of(first, block), block)
        scores = dot_nt(k_ref[rows, :], query) * LOG2_SCALE
        if masked:
            pairs = seen(pc_ref[rows, :], sc_ref[rows, :], pr_ref[...], sr_ref[...])
            scores = jnp.where(pairs, scores, MASKED_SCORE)
        new_top = jnp.maximum(top, jnp.max(scores, axis=0, keepdims=True))
        fade = jnp.exp2(top - new_top)
        probs = jnp.exp2(scores - new_top)
        total = total * fade + jnp.sum(probs, axis=0, keepdims=True)
        acc = acc * fade + dot_nn(vt_ref[:, rows], probs.astype(jnp.bfloat16))
        return new_top, total, acc

    state = (
        jnp.full((1, block), MASKED_SCORE, jnp.float32),
        jnp.zeros((1, block), jnp.float32),
        jnp.zeros((HDIM, block), jnp.float32),
    )
    state = lax.fori_loop(0, index, lambda j, s: step(j * block, s, False), state)
    top, total, acc = step(index * block, state, True)
    o_ref[...] = (acc / total).T.astype(jnp.bfloat16)
    l_ref[0] = top + jnp.log2(total)

def attend(q, k, v, pos, seg, block=512):
    rows, cols = q.shape
    heads = cols // HDIM
    grid = (heads, rows // block)
    tile = pl.BlockSpec((block, HDIM), lambda h, i: (i, h))
    whole = pl.BlockSpec((rows, HDIM), lambda h, i: (0, h))
    col = pl.BlockSpec((rows, 1), lambda h, i: (0, 0))
    row = pl.BlockSpec((1, block), lambda h, i: (0, i))
    return pl.pallas_call(
        functools.partial(attend_kernel, block),
        grid=grid,
        in_specs=[tile, whole, whole, col, col, row, row],
        out_specs=[tile, pl.BlockSpec((1, 1, block), lambda h, i: (h, 0, i))],
        out_shape=[
            jax.ShapeDtypeStruct((rows, cols), jnp.bfloat16),
            jax.ShapeDtypeStruct((heads, 1, rows), jnp.float32),
        ],
        scratch_shapes=[pltpu.VMEM((HDIM, rows), jnp.bfloat16)],
        cost_estimate=pl.CostEstimate(flops=30_000_000_000, bytes_accessed=4 * rows * cols * 2, transcendentals=0),
        name="attend",
    )(q, k, v, pos[:, None], seg[:, None], pos[None, :], seg[None, :])

def attend_back_kernel(block, q_ref, k_ref, v_ref, o_ref, go_ref, l_ref, pc_ref, sc_ref, pr_ref, sr_ref,
                       ck_ref, sk_ref, cq_ref, sq_ref, dq_ref, dk_ref, dv_ref, kt_ref, ak_ref, av_ref):
    index = pl.program_id(1)

    @pl.when(index == 0)
    def _():
        kt_ref[...] = k_ref[...].T

    query = q_ref[...]
    grad = go_ref[...]
    delta = jnp.sum((o_ref[...].astype(jnp.float32) * grad.astype(jnp.float32)).T, axis=0, keepdims=True)
    logs = l_ref[0]

    def step(first, acc, masked):
        rows = pl.ds(pl.multiple_of(first, block), block)
        scores = dot_nt(k_ref[rows, :], query) * LOG2_SCALE
        if masked:
            pairs = seen(pc_ref[rows, :], sc_ref[rows, :], pr_ref[...], sr_ref[...])
            scores = jnp.where(pairs, scores, MASKED_SCORE)
        probs = jnp.exp2(scores - logs)
        slopes = dot_nt(v_ref[rows, :], grad)
        turned = (probs * (slopes - delta)).astype(jnp.bfloat16)
        add_k = dot_nn(turned, query)
        add_v = dot_nn(probs.astype(jnp.bfloat16), grad)
        if masked:
            ak_ref[rows, :] = add_k
            av_ref[rows, :] = add_v
        else:
            ak_ref[rows, :] += add_k
            av_ref[rows, :] += add_v
        return acc + dot_nn(kt_ref[:, rows], turned)

    acc = lax.fori_loop(0, index, lambda j, s: step(j * block, s, False), jnp.zeros((HDIM, block), jnp.float32))
    acc = step(index * block, acc, True)

    def unturn(value, cosine, sine):
        value = value * SCORE_SCALE
        return (value * cosine - pltpu.roll(value, HDIM // 2, 1) * sine).astype(jnp.bfloat16)

    dq_ref[...] = unturn(acc.T, cq_ref[...], sq_ref[...])

    @pl.when(index == pl.num_programs(1) - 1)
    def _():
        @pl.loop(0, pl.num_programs(1))
        def _(j):
            rows = pl.ds(pl.multiple_of(j * block, block), block)
            dk_ref[rows, :] = unturn(ak_ref[rows, :], ck_ref[rows, :], sk_ref[rows, :])
            dv_ref[rows, :] = av_ref[rows, :].astype(jnp.bfloat16)

def attend_back(q, k, v, o, go, logs, pos, seg, cos2, sin2, block=512):
    rows, cols = q.shape
    heads = cols // HDIM
    grid = (heads, rows // block)
    tile = pl.BlockSpec((block, HDIM), lambda h, i: (i, h))
    whole = pl.BlockSpec((rows, HDIM), lambda h, i: (0, h))
    col = pl.BlockSpec((rows, 1), lambda h, i: (0, 0))
    row = pl.BlockSpec((1, block), lambda h, i: (0, i))
    table = pl.BlockSpec((rows, HDIM), lambda h, i: (0, 0))
    table_tile = pl.BlockSpec((block, HDIM), lambda h, i: (i, 0))
    like = jax.ShapeDtypeStruct((rows, cols), jnp.bfloat16)
    return pl.pallas_call(
        functools.partial(attend_back_kernel, block),
        grid=grid,
        in_specs=[tile, whole, whole, tile, tile, pl.BlockSpec((1, 1, block), lambda h, i: (h, 0, i)),
                  col, col, row, row, table, table, table_tile, table_tile],
        out_specs=[tile, whole, whole],
        out_shape=[like, like, like],
        scratch_shapes=[pltpu.VMEM((HDIM, rows), jnp.bfloat16), pltpu.VMEM((rows, HDIM), jnp.float32),
                        pltpu.VMEM((rows, HDIM), jnp.float32)],
        cost_estimate=pl.CostEstimate(flops=80_000_000_000, bytes_accessed=8 * rows * cols * 2, transcendentals=0),
        name="attend_back",
    )(q, k, v, o, go, logs, pos[:, None], seg[:, None], pos[None, :], seg[None, :], cos2, sin2, cos2, sin2)

EPSILON = 1e-05
HIGHEST_PRECISION = lax.Precision.HIGHEST
ROOT_HALF = math.sqrt(0.5)
PDF_SCALE = 1.0 / math.sqrt(2.0 * math.pi)

SCALAR = pl.BlockSpec(memory_space=pltpu.SMEM)


def gelu_pair(u):
    cdf = 0.5 + 0.5 * lax.erf(u * ROOT_HALF)
    return u * cdf, cdf + u * (PDF_SCALE * jnp.exp(-0.5 * u * u))

def exact_dot(a, b, dims):
    return lax.dot_general(a, b, (dims, ((), ())), precision=HIGHEST_PRECISION, preferred_element_type=jnp.float32)

def low_dot(a, b, dims):
    return lax.dot_general(a, b, (dims, ((), ())), preferred_element_type=jnp.float32)

def standard(x):
    width = x.shape[-1]
    centre = x - jnp.sum(x, axis=-1, keepdims=True) * (1.0 / width)
    spread = jnp.sum(centre * centre, axis=-1, keepdims=True) * (1.0 / width)
    rstd = lax.rsqrt(spread + EPSILON)
    return centre * rstd, rstd

def pull_standard(xhat, rstd, w):
    width = xhat.shape[-1]
    mean_w = jnp.sum(w, axis=-1, keepdims=True) * (1.0 / width)
    mean_wx = jnp.sum(w * xhat, axis=-1, keepdims=True) * (1.0 / width)
    return (w - mean_w - xhat * mean_wx) * rstd

def row_tile(rows, most):
    tile = min(most, rows)
    while rows % tile:
        tile -= 16
    return tile

def chunk_starts(core, width, owners):
    size = width // owners
    return [
        (o * size, pl.multiple_of((core ^ (o % 2)) * (width // 2) + (o // 2) * size, size))
        for o in range(owners)
    ]


def store_halves(ref, value, core, owners):
    size = value.shape[1] // owners
    for first, target in chunk_starts(core, value.shape[1], owners):
        ref[:, pl.ds(target, size)] = value[:, first : first + size]


def load_halves(ref, core, owners):
    width = ref.shape[1]
    size = width // owners
    return jnp.concatenate(
        [ref[:, pl.ds(target, size)] for _, target in chunk_starts(core, width, owners)], axis=1
    )


def norm_kernel(owners, core_ref, x_ref, gain_ref, shift_ref, n_ref):
    xhat, _ = standard(x_ref[0].astype(jnp.float32))
    value = (xhat * gain_ref[0] + shift_ref[0]).astype(jnp.bfloat16)
    store_halves(n_ref.at[0], value, core_ref[0], owners)

def norm_streams(x, count, gains, shifts, core, owners):
    rows, width = x.shape[1:]
    tile = row_tile(rows, 128)
    block = pl.BlockSpec((1, tile, width), lambda s, i: (s, i, 0))
    vec = pl.BlockSpec((1, 1, width), lambda s, i: (s, 0, 0))
    return pl.pallas_call(
        functools.partial(norm_kernel, owners), grid=(count, rows // tile),
        in_specs=[SCALAR, block, vec, vec], out_specs=block,
        out_shape=jax.ShapeDtypeStruct((count, rows, width), jnp.bfloat16), name="norm_streams",
    )(core, x, gains[:, None, :], shifts[:, None, :])

def add_parts(part_ref, halves, switch):
    low = pl.program_id(0) < switch
    total = part_ref[...].astype(jnp.float32)
    for first, second in (halves[:2], halves[2:]):
        total = total + jnp.where(
            low, first[...].astype(jnp.float32), second[...].astype(jnp.float32)
        )
    return total


def half_specs(tile, width, switch):
    first = pl.BlockSpec((tile, width), lambda i: (jnp.minimum(i, switch - 1), 0))
    second = pl.BlockSpec((tile, width), lambda i: (jnp.maximum(i - switch, 0), 0))
    return [first, second, first, second]


def mixer_kernel(switch, mid_ref, part_ref, xl_ref, xh_ref, yl_ref, yh_ref, prior_ref, up_ref, gain_ref, shift_ref,
                 mixin_ref, mixout_ref, bias_ref,
                 new_ref, gprior_ref, gout_ref, gz_ref, gin_ref, gmo_ref, gmb_ref, gg_ref, gs_ref):
    first = pl.program_id(0) == 0
    sources = prior_ref.shape[0] + 1
    count = up_ref.shape[0]
    tile = mid_ref.shape[0]
    wide = count * sources
    out = mid_ref[...] + add_parts(part_ref, (xl_ref, xh_ref, yl_ref, yh_ref), switch)
    xhat, rstd = standard(out)
    gain = gain_ref[...]
    c = (xhat * gain + shift_ref[...]).astype(jnp.bfloat16)
    g = low_dot(c, mixin_ref[...], ((1,), (1,)))
    act, slope = gelu_pair(g)
    coef = exact_dot(act, mixout_ref[...], ((1,), (0,))) + bias_ref[...]
    x = [prior_ref[j].astype(jnp.float32) for j in range(sources - 1)] + [out]
    u = [up_ref[s].astype(jnp.float32) for s in range(count)]
    co = [[coef[:, s * sources + j : s * sources + j + 1] for j in range(sources)] for s in range(count)]
    lane = lax.broadcasted_iota(jnp.int32, (tile, wide), 1)
    gcoef = jnp.zeros((tile, wide), jnp.float32)
    for s in range(count):
        mixed = co[s][0] * x[0]
        for j in range(1, sources):
            mixed = mixed + co[s][j] * x[j]
        new_ref[s] = mixed.astype(jnp.bfloat16)
        for j in range(sources):
            inner = jnp.sum(u[s] * x[j], axis=-1, keepdims=True)
            gcoef = jnp.where(lane == s * sources + j, inner, gcoef)
    for j in range(sources):
        total = co[0][j] * u[0]
        for s in range(1, count):
            total = total + co[s][j] * u[s]
        if j < sources - 1:
            gprior_ref[j] = total.astype(jnp.bfloat16)
    gact = exact_dot(gcoef, mixout_ref[...], ((1,), (1,)))
    gg = (gact * slope).astype(jnp.bfloat16)
    gc = low_dot(gg, mixin_ref[...], ((1,), (0,)))
    gout = total + pull_standard(xhat, rstd, gc * gain)
    gout_ref[...] = gout
    gz_ref[...] = gout.astype(jnp.bfloat16)

    @pl.when(first)
    def _():
        for ref in (gin_ref, gmo_ref, gmb_ref, gg_ref, gs_ref):
            ref[...] = jnp.zeros_like(ref)

    gin_ref[...] += low_dot(gg, c, ((0,), (0,)))
    gmo_ref[...] += exact_dot(act, gcoef, ((0,), (0,)))
    gmb_ref[...] += jnp.sum(gcoef, axis=0, keepdims=True)
    gg_ref[...] += jnp.sum(gc * xhat, axis=0, keepdims=True)
    gs_ref[...] += jnp.sum(gc, axis=0, keepdims=True)

def mixer(mid, parts, prior, d_streams, gain, shift, mix_in, mix_out, mix_bias, most=64):
    rows, width = mid.shape
    hidden = mix_in.shape[0]
    wide = mix_out.shape[1]
    tile = row_tile(rows // 2, most)
    switch = rows // 2 // tile
    flat = pl.BlockSpec((tile, width), lambda i: (i, 0))
    stack = lambda n: pl.BlockSpec((n, tile, width), lambda i: (0, i, 0))
    full = lambda *s: pl.BlockSpec(s, lambda i: (0,) * len(s))
    f32 = jnp.float32
    shape = jax.ShapeDtypeStruct
    return pl.pallas_call(
        functools.partial(mixer_kernel, switch), grid=(rows // tile,),
        in_specs=[flat, flat, *half_specs(tile, width, switch), stack(prior.shape[0]), stack(d_streams.shape[0]),
                  full(1, width), full(1, width), full(hidden, width), full(hidden, wide), full(1, wide)],
        out_specs=[stack(d_streams.shape[0]), stack(prior.shape[0]), flat, flat,
                   full(hidden, width), full(hidden, wide), full(1, wide), full(1, width), full(1, width)],
        out_shape=[shape(d_streams.shape, jnp.bfloat16), shape(prior.shape, jnp.bfloat16),
                   shape((rows, width), f32), shape((rows, width), jnp.bfloat16),
                   shape((hidden, width), f32), shape((hidden, wide), f32), shape((1, wide), f32),
                   shape((1, width), f32), shape((1, width), f32)],
        cost_estimate=pl.CostEstimate(flops=1000000, bytes_accessed=60_000_000, transcendentals=0),
        name="mixer",
    )(mid, *parts, prior, d_streams, gain[None], shift[None], mix_in, mix_out, mix_bias[None])

def middle_kernel(owners, core_ref, attn_ref, stream_ref, gain_ref, shift_ref, mid_ref, m_ref):
    mid = load_halves(attn_ref, core_ref[0], owners) + stream_ref[0].astype(jnp.float32)
    mid_ref[...] = mid
    xhat, _ = standard(mid)
    m_ref[...] = (xhat * gain_ref[...] + shift_ref[...]).astype(jnp.bfloat16)

def middle(attn, streams, gain, shift, core, owners):
    rows, width = attn.shape
    tile = row_tile(rows, 128)
    flat = pl.BlockSpec((tile, width), lambda i: (i, 0))
    vec = pl.BlockSpec((1, width), lambda i: (0, 0))
    return pl.pallas_call(
        functools.partial(middle_kernel, owners), grid=(rows // tile,),
        in_specs=[SCALAR, flat, pl.BlockSpec((1, tile, width), lambda i: (3, i, 0)), vec, vec],
        out_specs=[flat, flat],
        out_shape=[jax.ShapeDtypeStruct((rows, width), jnp.float32), jax.ShapeDtypeStruct((rows, width), jnp.bfloat16)],
        name="middle",
    )(core, attn, streams, gain[None], shift[None])

def middle_back(mid, gout, parts, gain, core, owners):
    rows, width = mid.shape
    tile = row_tile(rows // 2, 64)
    switch = rows // 2 // tile
    flat = pl.BlockSpec((tile, width), lambda i: (i, 0))
    vec = pl.BlockSpec((1, width), lambda i: (0, 0))
    shape = jax.ShapeDtypeStruct
    return pl.pallas_call(
        functools.partial(middle_back_kernel, owners, switch), grid=(rows // tile,),
        in_specs=[SCALAR] + [flat] * 3 + half_specs(tile, width, switch) + [vec], out_specs=[flat, vec, vec],
        out_shape=[shape((rows, width), jnp.bfloat16), shape((1, width), jnp.float32), shape((1, width), jnp.float32)],
        name="middle_back",
    )(core, mid, gout, *parts, gain[None])

def middle_back_kernel(owners, switch, core_ref, mid_ref, gout_ref, part_ref, xl_ref, xh_ref, yl_ref, yh_ref, gain_ref, low_ref, gg_ref, gs_ref):
    xhat, rstd = standard(mid_ref[...])
    r = add_parts(part_ref, (xl_ref, xh_ref, yl_ref, yh_ref), switch)
    value = (gout_ref[...] + pull_standard(xhat, rstd, r * gain_ref[...])).astype(jnp.bfloat16)
    store_halves(low_ref, value, core_ref[0], owners)

    @pl.when(pl.program_id(0) == 0)
    def _():
        gg_ref[...] = jnp.zeros_like(gg_ref)
        gs_ref[...] = jnp.zeros_like(gs_ref)

    gg_ref[...] += jnp.sum(r * xhat, axis=0, keepdims=True)
    gs_ref[...] += jnp.sum(r, axis=0, keepdims=True)

def streams_back_kernel(owners, core_ref, x_ref, rq_ref, rk_ref, rv_ref, last_ref, gain_ref, gx_ref, gg_ref, gs_ref):
    @pl.when(pl.program_id(0) == 0)
    def _():
        gg_ref[...] = jnp.zeros_like(gg_ref)
        gs_ref[...] = jnp.zeros_like(gs_ref)

    for s, ref in enumerate((rq_ref, rk_ref, rv_ref)):
        xhat, rstd = standard(x_ref[s].astype(jnp.float32))
        r = load_halves(ref, core_ref[0], owners)
        gx_ref[s] = pull_standard(xhat, rstd, r * gain_ref[s]).astype(jnp.bfloat16)
        gg_ref[s] += jnp.sum(r * xhat, axis=0, keepdims=True)
        gs_ref[s] += jnp.sum(r, axis=0, keepdims=True)
    gx_ref[3] = load_halves(last_ref, core_ref[0], owners)

def streams_back(x, rq, rk, rv, last, gains, core, owners):
    rows, width = rq.shape
    tile = row_tile(rows, 64)
    flat = pl.BlockSpec((tile, width), lambda i: (i, 0))
    three = pl.BlockSpec((3, 1, width), lambda i: (0, 0, 0))
    shape = jax.ShapeDtypeStruct
    return pl.pallas_call(
        functools.partial(streams_back_kernel, owners), grid=(rows // tile,),
        in_specs=[SCALAR, pl.BlockSpec((3, tile, width), lambda i: (0, i, 0)), flat, flat, flat, flat, three],
        out_specs=[pl.BlockSpec((4, tile, width), lambda i: (0, i, 0)), three, three],
        out_shape=[shape((4, rows, width), jnp.bfloat16), shape((3, 1, width), jnp.float32), shape((3, 1, width), jnp.float32)],
        name="streams_back",
    )(core, x, rq, rk, rv, last, gains[:, None, :])


def project_kernel(turn, swap, place_ref, n_ref, mine_ref, other_ref, *rest):
    dims = ((1,), (1 if swap else 0,))
    half = n_ref.shape[1] // 2
    y = low_dot(n_ref[:, :half], mine_ref[0], dims) + low_dot(n_ref[:, half:], other_ref[0], dims)
    o_ref = rest[-1]
    if turn:
        c_ref, s_ref = rest[:2]
        for h in range(y.shape[1] // HDIM):
            cols = slice(h * HDIM, (h + 1) * HDIM)
            part = y[:, cols]
            part = part * c_ref[...] + pltpu.roll(part, HDIM // 2, 1) * s_ref[...]
            o_ref[0, :, cols] = part.astype(jnp.bfloat16)
    else:
        o_ref[0] = y.astype(jnp.bfloat16)


def project(n, halves, place, tables=(), swap=False, name="project"):
    rows, width = n.shape
    groups = halves[0].shape[0]
    cols = halves[0].shape[1 if swap else 2]
    part = pl.BlockSpec((1,) + halves[0].shape[1:], lambda r, p: (r, 0, 0))
    table = pl.BlockSpec((rows, HDIM), lambda r, p: (0, 0))
    return pl.pallas_call(
        functools.partial(project_kernel, bool(tables), swap),
        grid_spec=pltpu.PrefetchScalarGridSpec(
            num_scalar_prefetch=1,
            grid=(groups,),
            in_specs=[pl.BlockSpec((rows, width), lambda r, p: (0, 0)), part, part]
            + [table] * len(tables),
            out_specs=pl.BlockSpec((1, rows, cols), lambda r, p: (p[0] ^ r, 0, 0)),
        ),
        out_shape=jax.ShapeDtypeStruct((groups, rows, cols), jnp.bfloat16),
        cost_estimate=pl.CostEstimate(
            flops=2 * rows * width * cols * groups,
            bytes_accessed=2 * width * cols * groups,
            transcendentals=0,
        ),
        name=name,
    )(place, n, *halves, *tables)


def join_kernel(swap, tiles, place_ref, a_ref, mine_ref, other_ref, o_ref):
    place = place_ref[0]

    def add_up(w_ref):
        total = None
        for r in range(a_ref.shape[0]):
            part = low_dot(a_ref[place ^ r], w_ref[r], ((1,), (1 if swap else 0,)))
            total = part if total is None else total + part
        o_ref[...] = total

    index = pl.program_id(0)
    pl.when(index < tiles)(lambda: add_up(mine_ref))
    pl.when(index >= tiles)(lambda: add_up(other_ref))


def join(a, halves, place, swap=False, name="join"):
    groups, rows, cols = a.shape
    half = halves[0].shape[1 if swap else 2]
    tile = 512
    tiles = half // tile

    def spec(place_of):
        if swap:
            return pl.BlockSpec((groups, tile, cols), lambda i, p: (0, place_of(i), 0))
        return pl.BlockSpec((groups, cols, tile), lambda i, p: (0, 0, place_of(i)))

    return pl.pallas_call(
        functools.partial(join_kernel, swap, tiles),
        grid_spec=pltpu.PrefetchScalarGridSpec(
            num_scalar_prefetch=1,
            grid=(2 * tiles,),
            in_specs=[
                pl.BlockSpec((groups, rows, cols), lambda i, p: (0, 0, 0)),
                spec(lambda i: jnp.minimum(i, tiles - 1)),
                spec(lambda i: jnp.maximum(i - tiles, 0)),
            ],
            out_specs=pl.BlockSpec((rows, tile), lambda i, p: (0, i)),
        ),
        out_shape=jax.ShapeDtypeStruct((rows, 2 * half), jnp.float32),
        cost_estimate=pl.CostEstimate(
            flops=4 * rows * half * cols * groups,
            bytes_accessed=4 * half * cols * groups,
            transcendentals=0,
        ),
        name=name,
    )(place, a, *halves)


def weight_kernel(swap, place_ref, n_ref, a_ref, mine_ref, other_ref, t_ref):
    dims = ((1,), (0,))
    half = n_ref.shape[1] // 2
    if swap:
        turned = a_ref[0].T
        mine_ref[0] = low_dot(turned, n_ref[:, :half], dims).astype(jnp.bfloat16)
        other_ref[0] = low_dot(turned, n_ref[:, half:], dims).astype(jnp.bfloat16)
    else:
        @pl.when(pl.program_id(0) == 0)
        def _():
            t_ref[...] = n_ref[...].T

        mine_ref[0] = low_dot(t_ref[:half], a_ref[0], dims).astype(jnp.bfloat16)
        other_ref[0] = low_dot(t_ref[half:], a_ref[0], dims).astype(jnp.bfloat16)


def weight_grad(n, a, place, swap=False, name="weight_grad"):
    rows, width = n.shape
    groups, _, cols = a.shape
    half = width // 2
    out = (cols, half) if swap else (half, cols)
    part = pl.BlockSpec((1,) + out, lambda r, p: (r, 0, 0))
    return pl.pallas_call(
        functools.partial(weight_kernel, swap),
        grid_spec=pltpu.PrefetchScalarGridSpec(
            num_scalar_prefetch=1,
            grid=(groups,),
            in_specs=[
                pl.BlockSpec((rows, width), lambda r, p: (0, 0)),
                pl.BlockSpec((1, rows, cols), lambda r, p: (p[0] ^ r, 0, 0)),
            ],
            out_specs=[part, part],
            scratch_shapes=[pltpu.VMEM((16, 128) if swap else (width, rows), jnp.bfloat16)],
        ),
        out_shape=[jax.ShapeDtypeStruct((groups,) + out, jnp.bfloat16)] * 2,
        cost_estimate=pl.CostEstimate(
            flops=2 * rows * width * cols * groups,
            bytes_accessed=2 * width * cols * groups,
            transcendentals=0,
        ),
        name=name,
    )(place, n, a)


def rotary_tables(position_row):
    half_width = HDIM // 2
    frequency = jnp.exp(
        jnp.arange(half_width, dtype=jnp.float32) * (-2.0 * math.log(10000.0) / HDIM)
    )
    angles = position_row.astype(jnp.float32)[:, None] * frequency[None, :]
    cosine, sine = jnp.cos(angles), jnp.sin(angles)
    return jnp.concatenate([cosine, cosine], axis=1), jnp.concatenate([-sine, sine], axis=1)


def hop(value, mask):
    size = lax.axis_size("tensor")
    return lax.ppermute(value, "tensor", [(i, i ^ mask) for i in range(size)])


def spread_rows(own):
    if lax.axis_size("tensor") != 4:
        return [lax.all_gather(own, "tensor", axis=0, tiled=True)]
    half = own.shape[0] // 2
    one, two = hop(own, 1), hop(own, 2)
    return [own, one, two, hop(one[:half], 2), hop(two[half:], 1)]


def add_low(left, right):
    return (left.astype(jnp.float32) + right.astype(jnp.float32)).astype(jnp.bfloat16)


def collect_rows(pieces):
    if lax.axis_size("tensor") != 4:
        total = lax.psum_scatter(pieces[0], "tensor", scatter_dimension=0, tiled=True)
        zero = jnp.zeros_like(total[: total.shape[0] // 2])
        return total, zero, zero, zero, zero
    own, one, two, far_low, far_high = pieces
    half = own.shape[0] // 2
    one_low = hop(one[:half], 1)
    two_high = hop(two[half:], 2)
    low = hop(far_low, 1)
    high = hop(far_high, 2)
    one_high = hop(add_low(one[half:], high), 1)
    two_low = hop(add_low(two[:half], low), 2)
    return own, one_low, one_high, two_low, two_high


def sum_all(value):
    for axis in ("tensor", "dp"):
        size = lax.axis_size(axis)
        bit = 1
        while bit < size:
            value = value + lax.ppermute(value, axis, [(i, i ^ bit) for i in range(size)])
            bit *= 2
    return value


def exchange(value):
    return lax.all_to_all(value, "tensor", split_axis=0, concat_axis=0, tiled=True)


def reorder(value):
    size = lax.axis_size("tensor")
    return value[jnp.arange(size, dtype=jnp.int32) ^ lax.axis_index("tensor")]


def return_heads(value):
    if lax.axis_size("tensor") != 4:
        return reorder(exchange(value))
    place = lax.axis_index("tensor")
    blocks = [lax.dynamic_index_in_dim(value, place ^ r, 0, keepdims=False) for r in range(4)]
    return jnp.stack([blocks[0]] + [hop(blocks[r], r) for r in (1, 2, 3)])


def core_groups():
    size = lax.axis_size("dp")
    return [list(range(core, size, 2)) for core in (0, 1)]


def core_hop(value):
    size = lax.axis_size("dp")
    return lax.ppermute(value, "dp", [(i, i ^ 1) for i in range(size)])


def gather_lane(shards, axis):
    return lax.all_gather(shards, "dp", axis=axis, tiled=True, axis_index_groups=core_groups())


def gather_plane(lane):
    if lax.axis_size("tensor") == 4:
        own, one, two, low, high = spread_rows(lane)
        mine = jnp.stack([own, one, two, jnp.concatenate([low, high])])
    else:
        mine = reorder(lax.all_gather(lane, "tensor", axis=0, tiled=False))
    return mine, core_hop(mine)


def reduce_core(halves):
    mine, other = halves
    return add_low(mine, core_hop(other))


def reduce_plane(total):
    if lax.axis_size("tensor") != 4:
        return lax.psum_scatter(reorder(total), "tensor", scatter_dimension=0, tiled=False)
    half = total.shape[1] // 2
    own, *rest = collect_rows([total[0], total[1], total[2], total[3, :half], total[3, half:]])
    one_low, one_high, two_low, two_high = (x.astype(jnp.float32) for x in rest)
    own = own.astype(jnp.float32)
    return jnp.concatenate(
        [own[:half] + one_low + two_low, own[half:] + one_high + two_high]
    ).astype(jnp.bfloat16)


def reduce_lane(value, axis):
    return lax.psum_scatter(
        value, "dp", scatter_dimension=axis, tiled=True, axis_index_groups=core_groups()
    ).astype(jnp.float32)


def contract_first(left, right):
    return low_dot(left, right, ((0,), (0,)))


def contract_last(left, right):
    return low_dot(left, right, ((1,), (1,)))


def split_columns(value):
    size = lax.axis_size("dp")
    rows, cols = value.shape
    return value.reshape(rows, size, cols // size).transpose(1, 0, 2).reshape(size, -1)


def reduce_small(values):
    size = lax.axis_size("dp")
    packed = jnp.concatenate([split_columns(value) for value in values], axis=1)
    length = packed.shape[1]
    rows = -(-length // 1024) * 8
    packed = jnp.pad(packed, ((0, 0), (0, rows * 128 - length))).reshape(size, rows, 128)
    mine = lax.dynamic_index_in_dim(
        sum_all(packed), lax.axis_index("dp"), 0, keepdims=False
    ).reshape(-1)
    result, first = [], 0
    for value in values:
        count = value.shape[0] * value.shape[1] // size
        result.append(mine[first : first + count].reshape(value.shape[0], -1))
        first += count
    return result


def gather_small(values):
    size = lax.axis_size("dp")
    packed = jnp.concatenate([value.reshape(-1) for value in values])
    length = packed.shape[0]
    rows = -(-length // 2048) * 16
    packed = jnp.pad(packed, (0, rows * 128 - length)).reshape(rows, 128)
    every = lax.all_gather(packed, "dp", axis=0, tiled=False).reshape(size, -1)
    result, first = [], 0
    for value in values:
        count = value.size
        block = every[:, first : first + count].reshape(size, value.shape[0], -1)
        result.append(block.transpose(1, 0, 2).reshape(value.shape[0], -1))
        first += count
    return result


def body(
    streams,
    prior,
    seg_ids,
    positions,
    w_qk,
    w_value,
    w_out,
    w_up,
    w_down,
    norm_gain,
    norm_bias,
    mix_in,
    mix_out,
    mix_bias,
    d_streams,
):
    rows_dev = streams.shape[1]
    bf16 = jnp.bfloat16
    gains, shifts, mixin_cols, mixout_all, mixbias_all = gather_small(
        [norm_gain, norm_bias, mix_in.T, mix_out, mix_bias[None]]
    )
    gains, shifts = gains.astype(jnp.float32), shifts.astype(jnp.float32)
    mixout_all, mixbias_all = mixout_all.astype(jnp.float32), mixbias_all.astype(jnp.float32)
    owners = lax.axis_size("dp")
    core = (lax.axis_index("dp") % 2).astype(jnp.int32)[None]
    place = lax.axis_index("tensor").astype(jnp.int32)
    here, still = place[None], jnp.zeros((1,), jnp.int32)
    lanes = [gather_lane(w, 0) for w in (w_qk[0], w_qk[1], w_value)]
    query_full, key_full, value_full = (gather_plane(lane) for lane in lanes)
    w_out, w_up = lax.optimization_barrier((w_out, w_up, lanes))[:2]
    lane_out = gather_lane(w_out, 1)
    up_all = lax.all_gather(w_up, "dp", axis=0, tiled=True)
    w_down = lax.optimization_barrier((w_down, up_all))[0]
    down_all = lax.all_gather(w_down, "dp", axis=1, tiled=True)

    tables = rotary_tables(positions)
    own_tables = [lax.dynamic_slice_in_dim(t, place * rows_dev, rows_dev) for t in tables]
    normed = norm_streams(streams, 3, gains[:3], shifts[:3], core, owners)
    query = exchange(project(normed[0], query_full, here, own_tables, name="query"))
    key = exchange(project(normed[1], key_full, here, own_tables, name="key"))
    value = exchange(project(normed[2], value_full, here, name="value"))
    heads_shape = (value.shape[0] * value.shape[1], value.shape[2])
    query, key, value = (x.reshape(heads_shape) for x in (query, key, value))
    lane_out = lax.optimization_barrier((lane_out, value))[0]
    out_full = gather_plane(lane_out)
    attended, logs = attend(query, key, value, positions, seg_ids)
    attended_rows = exchange(attended.reshape(-1, rows_dev, heads_shape[1]))
    attn_result = join(attended_rows, out_full, here, name="attn_out")
    mid, mlp_input = middle(attn_result, streams, gains[3], shifts[3], core, owners)

    mlp_rows = spread_rows(mlp_input)
    hidden, slopes, parts = [], [], []
    for rows in mlp_rows:
        acts, slope = gelu_pair(low_dot(rows, up_all, ((1,), (0,))))
        hidden.append(acts.astype(bf16))
        slopes.append(slope.astype(bf16))
        parts.append(low_dot(hidden[-1], down_all, ((1,), (0,))).astype(bf16))
    parts = collect_rows(parts)
    (
        new_streams,
        grad_prior,
        grad_layer,
        grad_layer_low,
        grad_mix_in,
        grad_mix_out,
        grad_mix_bias,
        gain_four,
        shift_four,
    ) = mixer(
        mid, parts, prior, d_streams, gains[4], shifts[4], mixin_cols, mixout_all, mixbias_all[0]
    )

    grad_rows = spread_rows(grad_layer_low)
    grad_pre, parts = [], []
    for rows, slope in zip(grad_rows, slopes):
        grad_hidden = contract_last(rows, down_all)
        grad_pre.append((grad_hidden * slope.astype(jnp.float32)).astype(bf16))
        parts.append(contract_last(grad_pre[-1], up_all).astype(bf16))
    parts = collect_rows(parts)
    grad_w_down = contract_first(jnp.concatenate(hidden), jnp.concatenate(grad_rows)).astype(bf16)
    parts, grad_w_down = lax.optimization_barrier((parts, grad_w_down))
    shard_down = lax.psum_scatter(grad_w_down, "dp", scatter_dimension=1, tiled=True)
    grad_mid, gain_three, shift_three = middle_back(
        mid, grad_layer, parts, gains[3], core, owners
    )

    grad_attended = exchange(project(grad_mid, out_full, here, swap=True, name="attn_out_back"))
    grad_query, grad_key, grad_value = attend_back(
        query,
        key,
        value,
        attended,
        grad_attended.reshape(heads_shape),
        logs,
        positions,
        seg_ids,
        *tables,
    )
    grad_w_out = weight_grad(grad_mid, attended_rows, here, swap=True, name="grad_w_out")
    plane_out = reduce_plane(reduce_core(grad_w_out))
    mlp_rows, grad_query = lax.optimization_barrier((mlp_rows, grad_query))
    grad_w_up = contract_first(jnp.concatenate(mlp_rows), jnp.concatenate(grad_pre)).astype(bf16)
    shard_up = lax.psum_scatter(grad_w_up, "dp", scatter_dimension=0, tiled=True)
    rows, totals = [], []
    for normed_rows, grad in zip(normed, (grad_query, grad_key, grad_value)):
        rows.append(return_heads(grad.reshape(-1, rows_dev, heads_shape[1])))
        totals.append(reduce_core(weight_grad(normed_rows, rows[-1], still, name="grad_w_in")))
    rows, totals = lax.optimization_barrier((rows, totals))
    back = [
        join(part, full, still, swap=True, name="attn_in_back")
        for part, full in zip(rows, (query_full, key_full, value_full))
    ]
    grad_streams, gain_first, shift_first = streams_back(
        streams, *back, grad_mid, gains[:3], core, owners
    )
    planes = [reduce_plane(total) for total in totals]
    planes[0] = lax.optimization_barrier((planes[0], shard_down, shard_up))[0]
    shard_out = reduce_lane(plane_out, 1)
    shard_query, shard_key, shard_value = (reduce_lane(plane, 0) for plane in planes)
    late_gain, late_shift, total_mix_in, total_mix_out, total_mix_bias = reduce_small(
        [
            jnp.concatenate([gain_three, gain_four]),
            jnp.concatenate([shift_three, shift_four]),
            grad_mix_in,
            grad_mix_out,
            grad_mix_bias,
        ]
    )
    early_gain, early_shift = reduce_small([gain_first[:, 0], shift_first[:, 0]])
    return (
        new_streams,
        grad_streams,
        grad_prior,
        jnp.stack([shard_query, shard_key]),
        shard_value,
        shard_out,
        shard_up.astype(jnp.float32),
        shard_down.astype(jnp.float32),
        jnp.concatenate([early_gain, late_gain]),
        jnp.concatenate([early_shift, late_shift]),
        total_mix_in.T,
        total_mix_out,
        total_mix_bias[0],
    )


def solution(mesh):
    in_specs = (
        P(None, ("dp", "tensor"), None),
        P(None, ("dp", "tensor"), None),
        P("dp"),
        P("dp"),
        P(None, "dp", "tensor"),
        P("dp", "tensor"),
        P("tensor", "dp"),
        P("dp", "tensor"),
        P("tensor", "dp"),
        P(None, "dp"),
        P(None, "dp"),
        P("dp", None),
        P(None, "dp"),
        P("dp"),
        P(None, ("dp", "tensor"), None),
    )
    out_specs = (
        P(None, ("dp", "tensor"), None),
        P(None, ("dp", "tensor"), None),
        P(None, ("dp", "tensor"), None),
        P(None, "dp", "tensor"),
        P("dp", "tensor"),
        P("tensor", "dp"),
        P("dp", "tensor"),
        P("tensor", "dp"),
        P(None, "dp"),
        P(None, "dp"),
        P("dp", None),
        P(None, "dp"),
        P("dp"),
    )
    return jax.shard_map(body, mesh=mesh, in_specs=in_specs, out_specs=out_specs, check_vma=False)
```

```python
import functools
import math

import jax
import jax.numpy as jnp
from jax import lax
from jax.experimental import pallas as pl
from jax.experimental.pallas import tpu as pltpu
from jax.sharding import PartitionSpec as P

HDIM = 128
MASKED_SCORE = -1e30
SCORE_SCALE = 1.0 / math.sqrt(HDIM)
LOG2_SCALE = SCORE_SCALE * math.log2(math.e)

def dot_nt(a, b):
    return lax.dot_general(a, b, (((1,), (1,)), ((), ())), preferred_element_type=jnp.float32)

def dot_nn(a, b):
    return lax.dot_general(a, b, (((1,), (0,)), ((), ())), preferred_element_type=jnp.float32)

def seen(pos_col, seg_col, pos_row, seg_row):
    return ((seg_col == 0) | (seg_col == seg_row)) & (pos_col <= pos_row)

def attend_kernel(block, q_ref, k_ref, v_ref, pc_ref, sc_ref, pr_ref, sr_ref, o_ref, l_ref, vt_ref):
    index = pl.program_id(1)

    @pl.when(index == 0)
    def _():
        vt_ref[...] = v_ref[...].T

    query = q_ref[...]

    def step(first, state, masked):
        top, total, acc = state
        rows = pl.ds(pl.multiple_of(first, block), block)
        scores = dot_nt(k_ref[rows, :], query) * LOG2_SCALE
        if masked:
            pairs = seen(pc_ref[rows, :], sc_ref[rows, :], pr_ref[...], sr_ref[...])
            scores = jnp.where(pairs, scores, MASKED_SCORE)
        new_top = jnp.maximum(top, jnp.max(scores, axis=0, keepdims=True))
        fade = jnp.exp2(top - new_top)
        probs = jnp.exp2(scores - new_top)
        total = total * fade + jnp.sum(probs, axis=0, keepdims=True)
        acc = acc * fade + dot_nn(vt_ref[:, rows], probs.astype(jnp.bfloat16))
        return new_top, total, acc

    state = (
        jnp.full((1, block), MASKED_SCORE, jnp.float32),
        jnp.zeros((1, block), jnp.float32),
        jnp.zeros((HDIM, block), jnp.float32),
    )
    state = lax.fori_loop(0, index, lambda j, s: step(j * block, s, False), state)
    top, total, acc = step(index * block, state, True)
    o_ref[...] = (acc / total).T.astype(jnp.bfloat16)
    l_ref[0] = top + jnp.log2(total)

def attend(q, k, v, pos, seg, block=512):
    rows, cols = q.shape
    heads = cols // HDIM
    grid = (heads, rows // block)
    tile = pl.BlockSpec((block, HDIM), lambda h, i: (i, h))
    whole = pl.BlockSpec((rows, HDIM), lambda h, i: (0, h))
    col = pl.BlockSpec((rows, 1), lambda h, i: (0, 0))
    row = pl.BlockSpec((1, block), lambda h, i: (0, i))
    return pl.pallas_call(
        functools.partial(attend_kernel, block),
        grid=grid,
        in_specs=[tile, whole, whole, col, col, row, row],
        out_specs=[tile, pl.BlockSpec((1, 1, block), lambda h, i: (h, 0, i))],
        out_shape=[
            jax.ShapeDtypeStruct((rows, cols), jnp.bfloat16),
            jax.ShapeDtypeStruct((heads, 1, rows), jnp.float32),
        ],
        scratch_shapes=[pltpu.VMEM((HDIM, rows), jnp.bfloat16)],
        cost_estimate=pl.CostEstimate(flops=30_000_000_000, bytes_accessed=4 * rows * cols * 2, transcendentals=0),
        name="attend",
    )(q, k, v, pos[:, None], seg[:, None], pos[None, :], seg[None, :])

def attend_back_kernel(block, q_ref, k_ref, v_ref, o_ref, go_ref, l_ref, pc_ref, sc_ref, pr_ref, sr_ref,
                       ck_ref, sk_ref, cq_ref, sq_ref, dq_ref, dk_ref, dv_ref, kt_ref, ak_ref, av_ref):
    index = pl.program_id(1)

    @pl.when(index == 0)
    def _():
        kt_ref[...] = k_ref[...].T

    query = q_ref[...]
    grad = go_ref[...]
    delta = jnp.sum((o_ref[...].astype(jnp.float32) * grad.astype(jnp.float32)).T, axis=0, keepdims=True)
    logs = l_ref[0]

    def step(first, acc, masked):
        rows = pl.ds(pl.multiple_of(first, block), block)
        scores = dot_nt(k_ref[rows, :], query) * LOG2_SCALE
        if masked:
            pairs = seen(pc_ref[rows, :], sc_ref[rows, :], pr_ref[...], sr_ref[...])
            scores = jnp.where(pairs, scores, MASKED_SCORE)
        probs = jnp.exp2(scores - logs)
        slopes = dot_nt(v_ref[rows, :], grad)
        turned = (probs * (slopes - delta)).astype(jnp.bfloat16)
        add_k = dot_nn(turned, query)
        add_v = dot_nn(probs.astype(jnp.bfloat16), grad)
        if masked:
            ak_ref[rows, :] = add_k
            av_ref[rows, :] = add_v
        else:
            ak_ref[rows, :] += add_k
            av_ref[rows, :] += add_v
        return acc + dot_nn(kt_ref[:, rows], turned)

    acc = lax.fori_loop(0, index, lambda j, s: step(j * block, s, False), jnp.zeros((HDIM, block), jnp.float32))
    acc = step(index * block, acc, True)

    def unturn(value, cosine, sine):
        value = value * SCORE_SCALE
        return (value * cosine - pltpu.roll(value, HDIM // 2, 1) * sine).astype(jnp.bfloat16)

    dq_ref[...] = unturn(acc.T, cq_ref[...], sq_ref[...])

    @pl.when(index == pl.num_programs(1) - 1)
    def _():
        @pl.loop(0, pl.num_programs(1))
        def _(j):
            rows = pl.ds(pl.multiple_of(j * block, block), block)
            dk_ref[rows, :] = unturn(ak_ref[rows, :], ck_ref[rows, :], sk_ref[rows, :])
            dv_ref[rows, :] = av_ref[rows, :].astype(jnp.bfloat16)

def attend_back(q, k, v, o, go, logs, pos, seg, cos2, sin2, block=512):
    rows, cols = q.shape
    heads = cols // HDIM
    grid = (heads, rows // block)
    tile = pl.BlockSpec((block, HDIM), lambda h, i: (i, h))
    whole = pl.BlockSpec((rows, HDIM), lambda h, i: (0, h))
    col = pl.BlockSpec((rows, 1), lambda h, i: (0, 0))
    row = pl.BlockSpec((1, block), lambda h, i: (0, i))
    table = pl.BlockSpec((rows, HDIM), lambda h, i: (0, 0))
    table_tile = pl.BlockSpec((block, HDIM), lambda h, i: (i, 0))
    like = jax.ShapeDtypeStruct((rows, cols), jnp.bfloat16)
    return pl.pallas_call(
        functools.partial(attend_back_kernel, block),
        grid=grid,
        in_specs=[tile, whole, whole, tile, tile, pl.BlockSpec((1, 1, block), lambda h, i: (h, 0, i)),
                  col, col, row, row, table, table, table_tile, table_tile],
        out_specs=[tile, whole, whole],
        out_shape=[like, like, like],
        scratch_shapes=[pltpu.VMEM((HDIM, rows), jnp.bfloat16), pltpu.VMEM((rows, HDIM), jnp.float32),
                        pltpu.VMEM((rows, HDIM), jnp.float32)],
        cost_estimate=pl.CostEstimate(flops=80_000_000_000, bytes_accessed=8 * rows * cols * 2, transcendentals=0),
        name="attend_back",
    )(q, k, v, o, go, logs, pos[:, None], seg[:, None], pos[None, :], seg[None, :], cos2, sin2, cos2, sin2)

EPSILON = 1e-05
HIGHEST_PRECISION = lax.Precision.HIGHEST
ROOT_HALF = math.sqrt(0.5)
PDF_SCALE = 1.0 / math.sqrt(2.0 * math.pi)

SCALAR = pl.BlockSpec(memory_space=pltpu.SMEM)


def gelu_pair(u):
    cdf = 0.5 + 0.5 * lax.erf(u * ROOT_HALF)
    return u * cdf, cdf + u * (PDF_SCALE * jnp.exp(-0.5 * u * u))

def exact_dot(a, b, dims):
    return lax.dot_general(a, b, (dims, ((), ())), precision=HIGHEST_PRECISION, preferred_element_type=jnp.float32)

def low_dot(a, b, dims):
    return lax.dot_general(a, b, (dims, ((), ())), preferred_element_type=jnp.float32)

def standard(x):
    width = x.shape[-1]
    centre = x - jnp.sum(x, axis=-1, keepdims=True) * (1.0 / width)
    spread = jnp.sum(centre * centre, axis=-1, keepdims=True) * (1.0 / width)
    rstd = lax.rsqrt(spread + EPSILON)
    return centre * rstd, rstd

def pull_standard(xhat, rstd, w):
    width = xhat.shape[-1]
    mean_w = jnp.sum(w, axis=-1, keepdims=True) * (1.0 / width)
    mean_wx = jnp.sum(w * xhat, axis=-1, keepdims=True) * (1.0 / width)
    return (w - mean_w - xhat * mean_wx) * rstd

def row_tile(rows, most):
    tile = min(most, rows)
    while rows % tile:
        tile -= 16
    return tile

def chunk_starts(core, width, owners):
    size = width // owners
    return [
        (o * size, pl.multiple_of((core ^ (o % 2)) * (width // 2) + (o // 2) * size, size))
        for o in range(owners)
    ]


def store_halves(ref, value, core, owners):
    size = value.shape[1] // owners
    for first, target in chunk_starts(core, value.shape[1], owners):
        ref[:, pl.ds(target, size)] = value[:, first : first + size]


def load_halves(ref, core, owners):
    width = ref.shape[1]
    size = width // owners
    return jnp.concatenate(
        [ref[:, pl.ds(target, size)] for _, target in chunk_starts(core, width, owners)], axis=1
    )


def norm_kernel(owners, core_ref, x_ref, gain_ref, shift_ref, n_ref):
    xhat, _ = standard(x_ref[0].astype(jnp.float32))
    value = (xhat * gain_ref[0] + shift_ref[0]).astype(jnp.bfloat16)
    store_halves(n_ref.at[0], value, core_ref[0], owners)

def norm_streams(x, count, gains, shifts, core, owners):
    rows, width = x.shape[1:]
    tile = row_tile(rows, 128)
    block = pl.BlockSpec((1, tile, width), lambda s, i: (s, i, 0))
    vec = pl.BlockSpec((1, 1, width), lambda s, i: (s, 0, 0))
    return pl.pallas_call(
        functools.partial(norm_kernel, owners), grid=(count, rows // tile),
        in_specs=[SCALAR, block, vec, vec], out_specs=block,
        out_shape=jax.ShapeDtypeStruct((count, rows, width), jnp.bfloat16), name="norm_streams",
    )(core, x, gains[:, None, :], shifts[:, None, :])

def add_parts(part_ref, halves, switch):
    low = pl.program_id(0) < switch
    total = part_ref[...].astype(jnp.float32)
    for first, second in (halves[:2], halves[2:]):
        total = total + jnp.where(
            low, first[...].astype(jnp.float32), second[...].astype(jnp.float32)
        )
    return total


def half_specs(tile, width, switch):
    first = pl.BlockSpec((tile, width), lambda i: (jnp.minimum(i, switch - 1), 0))
    second = pl.BlockSpec((tile, width), lambda i: (jnp.maximum(i - switch, 0), 0))
    return [first, second, first, second]


def mixer_kernel(switch, mid_ref, part_ref, xl_ref, xh_ref, yl_ref, yh_ref, prior_ref, up_ref, gain_ref, shift_ref,
                 mixin_ref, mixout_ref, bias_ref,
                 new_ref, gprior_ref, gout_ref, gz_ref, gin_ref, gmo_ref, gmb_ref, gg_ref, gs_ref):
    first = pl.program_id(0) == 0
    sources = prior_ref.shape[0] + 1
    count = up_ref.shape[0]
    tile = mid_ref.shape[0]
    wide = count * sources
    out = mid_ref[...] + add_parts(part_ref, (xl_ref, xh_ref, yl_ref, yh_ref), switch)
    xhat, rstd = standard(out)
    gain = gain_ref[...]
    c = (xhat * gain + shift_ref[...]).astype(jnp.bfloat16)
    g = low_dot(c, mixin_ref[...], ((1,), (1,)))
    act, slope = gelu_pair(g)
    coef = exact_dot(act, mixout_ref[...], ((1,), (0,))) + bias_ref[...]
    x = [prior_ref[j].astype(jnp.float32) for j in range(sources - 1)] + [out]
    u = [up_ref[s].astype(jnp.float32) for s in range(count)]
    co = [[coef[:, s * sources + j : s * sources + j + 1] for j in range(sources)] for s in range(count)]
    lane = lax.broadcasted_iota(jnp.int32, (tile, wide), 1)
    gcoef = jnp.zeros((tile, wide), jnp.float32)
    for s in range(count):
        mixed = co[s][0] * x[0]
        for j in range(1, sources):
            mixed = mixed + co[s][j] * x[j]
        new_ref[s] = mixed.astype(jnp.bfloat16)
        for j in range(sources):
            inner = jnp.sum(u[s] * x[j], axis=-1, keepdims=True)
            gcoef = jnp.where(lane == s * sources + j, inner, gcoef)
    for j in range(sources):
        total = co[0][j] * u[0]
        for s in range(1, count):
            total = total + co[s][j] * u[s]
        if j < sources - 1:
            gprior_ref[j] = total.astype(jnp.bfloat16)
    gact = exact_dot(gcoef, mixout_ref[...], ((1,), (1,)))
    gg = (gact * slope).astype(jnp.bfloat16)
    gc = low_dot(gg, mixin_ref[...], ((1,), (0,)))
    gout = total + pull_standard(xhat, rstd, gc * gain)
    gout_ref[...] = gout
    gz_ref[...] = gout.astype(jnp.bfloat16)

    @pl.when(first)
    def _():
        for ref in (gin_ref, gmo_ref, gmb_ref, gg_ref, gs_ref):
            ref[...] = jnp.zeros_like(ref)

    gin_ref[...] += low_dot(gg, c, ((0,), (0,)))
    gmo_ref[...] += exact_dot(act, gcoef, ((0,), (0,)))
    gmb_ref[...] += jnp.sum(gcoef, axis=0, keepdims=True)
    gg_ref[...] += jnp.sum(gc * xhat, axis=0, keepdims=True)
    gs_ref[...] += jnp.sum(gc, axis=0, keepdims=True)

def mixer(mid, parts, prior, d_streams, gain, shift, mix_in, mix_out, mix_bias, most=64):
    rows, width = mid.shape
    hidden = mix_in.shape[0]
    wide = mix_out.shape[1]
    tile = row_tile(rows // 2, most)
    switch = rows // 2 // tile
    flat = pl.BlockSpec((tile, width), lambda i: (i, 0))
    stack = lambda n: pl.BlockSpec((n, tile, width), lambda i: (0, i, 0))
    full = lambda *s: pl.BlockSpec(s, lambda i: (0,) * len(s))
    f32 = jnp.float32
    shape = jax.ShapeDtypeStruct
    return pl.pallas_call(
        functools.partial(mixer_kernel, switch), grid=(rows // tile,),
        in_specs=[flat, flat, *half_specs(tile, width, switch), stack(prior.shape[0]), stack(d_streams.shape[0]),
                  full(1, width), full(1, width), full(hidden, width), full(hidden, wide), full(1, wide)],
        out_specs=[stack(d_streams.shape[0]), stack(prior.shape[0]), flat, flat,
                   full(hidden, width), full(hidden, wide), full(1, wide), full(1, width), full(1, width)],
        out_shape=[shape(d_streams.shape, jnp.bfloat16), shape(prior.shape, jnp.bfloat16),
                   shape((rows, width), f32), shape((rows, width), jnp.bfloat16),
                   shape((hidden, width), f32), shape((hidden, wide), f32), shape((1, wide), f32),
                   shape((1, width), f32), shape((1, width), f32)],
        cost_estimate=pl.CostEstimate(flops=1000000, bytes_accessed=60_000_000, transcendentals=0),
        name="mixer",
    )(mid, *parts, prior, d_streams, gain[None], shift[None], mix_in, mix_out, mix_bias[None])

def middle_kernel(attn_ref, stream_ref, gain_ref, shift_ref, mid_ref, m_ref):
    mid = attn_ref[...] + stream_ref[0].astype(jnp.float32)
    mid_ref[...] = mid
    xhat, _ = standard(mid)
    m_ref[...] = (xhat * gain_ref[...] + shift_ref[...]).astype(jnp.bfloat16)

def middle(attn, streams, gain, shift):
    rows, width = attn.shape
    tile = row_tile(rows, 128)
    flat = pl.BlockSpec((tile, width), lambda i: (i, 0))
    vec = pl.BlockSpec((1, width), lambda i: (0, 0))
    return pl.pallas_call(
        middle_kernel, grid=(rows // tile,),
        in_specs=[flat, pl.BlockSpec((1, tile, width), lambda i: (3, i, 0)), vec, vec],
        out_specs=[flat, flat],
        out_shape=[jax.ShapeDtypeStruct((rows, width), jnp.float32), jax.ShapeDtypeStruct((rows, width), jnp.bfloat16)],
        name="middle",
    )(attn, streams, gain[None], shift[None])

def middle_back(mid, gout, parts, gain):
    rows, width = mid.shape
    tile = row_tile(rows // 2, 64)
    switch = rows // 2 // tile
    flat = pl.BlockSpec((tile, width), lambda i: (i, 0))
    vec = pl.BlockSpec((1, width), lambda i: (0, 0))
    shape = jax.ShapeDtypeStruct
    return pl.pallas_call(
        functools.partial(middle_back_kernel, switch), grid=(rows // tile,),
        in_specs=[flat] * 3 + half_specs(tile, width, switch) + [vec], out_specs=[flat, vec, vec],
        out_shape=[shape((rows, width), jnp.bfloat16), shape((1, width), jnp.float32), shape((1, width), jnp.float32)],
        name="middle_back",
    )(mid, gout, *parts, gain[None])

def middle_back_kernel(switch, mid_ref, gout_ref, part_ref, xl_ref, xh_ref, yl_ref, yh_ref, gain_ref, low_ref, gg_ref, gs_ref):
    xhat, rstd = standard(mid_ref[...])
    r = add_parts(part_ref, (xl_ref, xh_ref, yl_ref, yh_ref), switch)
    value = (gout_ref[...] + pull_standard(xhat, rstd, r * gain_ref[...])).astype(jnp.bfloat16)
    low_ref[...] = value

    @pl.when(pl.program_id(0) == 0)
    def _():
        gg_ref[...] = jnp.zeros_like(gg_ref)
        gs_ref[...] = jnp.zeros_like(gs_ref)

    gg_ref[...] += jnp.sum(r * xhat, axis=0, keepdims=True)
    gs_ref[...] += jnp.sum(r, axis=0, keepdims=True)

def streams_back_kernel(owners, core_ref, x_ref, rq_ref, rk_ref, rv_ref, last_ref, gain_ref, gx_ref, gg_ref, gs_ref):
    @pl.when(pl.program_id(0) == 0)
    def _():
        gg_ref[...] = jnp.zeros_like(gg_ref)
        gs_ref[...] = jnp.zeros_like(gs_ref)

    for s, ref in enumerate((rq_ref, rk_ref, rv_ref)):
        xhat, rstd = standard(x_ref[s].astype(jnp.float32))
        r = load_halves(ref, core_ref[0], owners)
        gx_ref[s] = pull_standard(xhat, rstd, r * gain_ref[s]).astype(jnp.bfloat16)
        gg_ref[s] += jnp.sum(r * xhat, axis=0, keepdims=True)
        gs_ref[s] += jnp.sum(r, axis=0, keepdims=True)
    gx_ref[3] = last_ref[...]

def streams_back(x, rq, rk, rv, last, gains, core, owners):
    rows, width = rq.shape
    tile = row_tile(rows, 64)
    flat = pl.BlockSpec((tile, width), lambda i: (i, 0))
    three = pl.BlockSpec((3, 1, width), lambda i: (0, 0, 0))
    shape = jax.ShapeDtypeStruct
    return pl.pallas_call(
        functools.partial(streams_back_kernel, owners), grid=(rows // tile,),
        in_specs=[SCALAR, pl.BlockSpec((3, tile, width), lambda i: (0, i, 0)), flat, flat, flat, flat, three],
        out_specs=[pl.BlockSpec((4, tile, width), lambda i: (0, i, 0)), three, three],
        out_shape=[shape((4, rows, width), jnp.bfloat16), shape((3, 1, width), jnp.float32), shape((3, 1, width), jnp.float32)],
        name="streams_back",
    )(core, x, rq, rk, rv, last, gains[:, None, :])


def project_kernel(turn, swap, place_ref, n_ref, mine_ref, other_ref, *rest):
    dims = ((1,), (1 if swap else 0,))
    half = n_ref.shape[1] // 2
    y = low_dot(n_ref[:, :half], mine_ref[0], dims) + low_dot(n_ref[:, half:], other_ref[0], dims)
    o_ref = rest[-1]
    if turn:
        c_ref, s_ref = rest[:2]
        for h in range(y.shape[1] // HDIM):
            cols = slice(h * HDIM, (h + 1) * HDIM)
            part = y[:, cols]
            part = part * c_ref[...] + pltpu.roll(part, HDIM // 2, 1) * s_ref[...]
            o_ref[0, :, cols] = part.astype(jnp.bfloat16)
    else:
        o_ref[0] = y.astype(jnp.bfloat16)


def project(n, halves, place, tables=(), swap=False, name="project"):
    rows, width = n.shape
    groups = halves[0].shape[0]
    cols = halves[0].shape[1 if swap else 2]
    if len(halves) == 1:
        halves = halves * 2
        parts = [
            pl.BlockSpec((1, cols, width // 2), lambda r, p: (r, 0, 0)),
            pl.BlockSpec((1, cols, width // 2), lambda r, p: (r, 0, 1)),
        ]
    else:
        parts = [pl.BlockSpec((1,) + halves[0].shape[1:], lambda r, p: (r, 0, 0))] * 2
    table = pl.BlockSpec((rows, HDIM), lambda r, p: (0, 0))
    return pl.pallas_call(
        functools.partial(project_kernel, bool(tables), swap),
        grid_spec=pltpu.PrefetchScalarGridSpec(
            num_scalar_prefetch=1,
            grid=(groups,),
            in_specs=[pl.BlockSpec((rows, width), lambda r, p: (0, 0)), *parts]
            + [table] * len(tables),
            out_specs=pl.BlockSpec((1, rows, cols), lambda r, p: (p[0] ^ r, 0, 0)),
        ),
        out_shape=jax.ShapeDtypeStruct((groups, rows, cols), jnp.bfloat16),
        cost_estimate=pl.CostEstimate(
            flops=2 * rows * width * cols * groups,
            bytes_accessed=2 * width * cols * groups,
            transcendentals=0,
        ),
        name=name,
    )(place, n, *halves, *tables)


def join_kernel(swap, tiles, place_ref, a_ref, mine_ref, other_ref, o_ref):
    place = place_ref[0]

    def add_up(w_ref):
        total = None
        for r in range(a_ref.shape[0]):
            part = low_dot(a_ref[place ^ r], w_ref[r], ((1,), (1 if swap else 0,)))
            total = part if total is None else total + part
        o_ref[...] = total

    index = pl.program_id(0)
    pl.when(index < tiles)(lambda: add_up(mine_ref))
    pl.when(index >= tiles)(lambda: add_up(other_ref))


def join(a, halves, place, swap=False, name="join"):
    groups, rows, cols = a.shape
    half = halves[0].shape[1 if swap else 2]
    tile = 512
    shift = 0
    if len(halves) == 1:
        halves = halves * 2
        half //= 2
        shift = half // tile
    tiles = half // tile

    def spec(place_of):
        if swap:
            return pl.BlockSpec((groups, tile, cols), lambda i, p: (0, place_of(i), 0))
        return pl.BlockSpec((groups, cols, tile), lambda i, p: (0, 0, place_of(i)))

    return pl.pallas_call(
        functools.partial(join_kernel, swap, tiles),
        grid_spec=pltpu.PrefetchScalarGridSpec(
            num_scalar_prefetch=1,
            grid=(2 * tiles,),
            in_specs=[
                pl.BlockSpec((groups, rows, cols), lambda i, p: (0, 0, 0)),
                spec(lambda i: jnp.minimum(i, tiles - 1)),
                spec(lambda i: jnp.maximum(i - tiles, 0) + shift),
            ],
            out_specs=pl.BlockSpec((rows, tile), lambda i, p: (0, i)),
        ),
        out_shape=jax.ShapeDtypeStruct((rows, 2 * half), jnp.float32),
        cost_estimate=pl.CostEstimate(
            flops=4 * rows * half * cols * groups,
            bytes_accessed=4 * half * cols * groups,
            transcendentals=0,
        ),
        name=name,
    )(place, a, *halves)


def head_grad_kernel(place_ref, n_ref, a_ref, o_ref):
    o_ref[0] = low_dot(a_ref[0].T, n_ref[...], ((1,), (0,))).astype(jnp.bfloat16)


def head_grad(n, a, place, name="head_grad"):
    rows, width = n.shape
    groups, _, cols = a.shape
    return pl.pallas_call(
        head_grad_kernel,
        grid_spec=pltpu.PrefetchScalarGridSpec(
            num_scalar_prefetch=1,
            grid=(groups,),
            in_specs=[
                pl.BlockSpec((rows, width), lambda r, p: (0, 0)),
                pl.BlockSpec((1, rows, cols), lambda r, p: (p[0] ^ r, 0, 0)),
            ],
            out_specs=pl.BlockSpec((1, cols, width), lambda r, p: (r, 0, 0)),
        ),
        out_shape=jax.ShapeDtypeStruct((groups, cols, width), jnp.bfloat16),
        cost_estimate=pl.CostEstimate(
            flops=2 * rows * width * cols * groups,
            bytes_accessed=2 * width * cols * groups,
            transcendentals=0,
        ),
        name=name,
    )(place, n, a)


def weight_kernel(place_ref, n_ref, a_ref, mine_ref, other_ref, t_ref):
    dims = ((1,), (0,))
    half = n_ref.shape[1] // 2

    @pl.when(pl.program_id(0) == 0)
    def _():
        t_ref[...] = n_ref[...].T

    mine_ref[0] = low_dot(t_ref[:half], a_ref[0], dims).astype(jnp.bfloat16)
    other_ref[0] = low_dot(t_ref[half:], a_ref[0], dims).astype(jnp.bfloat16)


def weight_grad(n, a, place, name="weight_grad"):
    rows, width = n.shape
    groups, _, cols = a.shape
    half = width // 2
    out = (half, cols)
    part = pl.BlockSpec((1,) + out, lambda r, p: (r, 0, 0))
    return pl.pallas_call(
        weight_kernel,
        grid_spec=pltpu.PrefetchScalarGridSpec(
            num_scalar_prefetch=1,
            grid=(groups,),
            in_specs=[
                pl.BlockSpec((rows, width), lambda r, p: (0, 0)),
                pl.BlockSpec((1, rows, cols), lambda r, p: (p[0] ^ r, 0, 0)),
            ],
            out_specs=[part, part],
            scratch_shapes=[pltpu.VMEM((width, rows), jnp.bfloat16)],
        ),
        out_shape=[jax.ShapeDtypeStruct((groups,) + out, jnp.bfloat16)] * 2,
        cost_estimate=pl.CostEstimate(
            flops=2 * rows * width * cols * groups,
            bytes_accessed=2 * width * cols * groups,
            transcendentals=0,
        ),
        name=name,
    )(place, n, a)


def after(value, *others):
    return lax.optimization_barrier((value, others))[0]


def rotary_tables(position_row):
    half_width = HDIM // 2
    frequency = jnp.exp(
        jnp.arange(half_width, dtype=jnp.float32) * (-2.0 * math.log(10000.0) / HDIM)
    )
    angles = position_row.astype(jnp.float32)[:, None] * frequency[None, :]
    cosine, sine = jnp.cos(angles), jnp.sin(angles)
    return jnp.concatenate([cosine, cosine], axis=1), jnp.concatenate([-sine, sine], axis=1)


def hop(value, mask):
    size = lax.axis_size("tensor")
    return lax.ppermute(value, "tensor", [(i, i ^ mask) for i in range(size)])


def spread_rows(own):
    if lax.axis_size("tensor") != 4:
        return [lax.all_gather(own, "tensor", axis=0, tiled=True)]
    half = own.shape[0] // 2
    one, two = hop(own, 1), hop(own, 2)
    return [own, one, two, hop(one[:half], 2), hop(two[half:], 1)]


def in_turn(pieces, parts):
    for index, piece in enumerate(pieces):
        if index == 1:
            piece = after(piece, pieces[2], parts[-1])
        elif index:
            piece = after(piece, parts[-1])
        yield piece


def add_low(left, right):
    return (left.astype(jnp.float32) + right.astype(jnp.float32)).astype(jnp.bfloat16)


def collect_rows(pieces):
    if lax.axis_size("tensor") != 4:
        total = lax.psum_scatter(pieces[0], "tensor", scatter_dimension=0, tiled=True)
        zero = jnp.zeros_like(total[: total.shape[0] // 2])
        return total, zero, zero, zero, zero
    own, one, two, far_low, far_high = pieces
    half = own.shape[0] // 2
    one_low = hop(one[:half], 1)
    two_high = hop(two[half:], 2)
    low = hop(far_low, 1)
    high = hop(far_high, 2)
    one_high = hop(add_low(one[half:], high), 1)
    two_low = hop(add_low(two[:half], low), 2)
    return own, one_low, one_high, two_low, two_high


def sum_all(value):
    for axis in ("tensor", "dp"):
        size = lax.axis_size(axis)
        bit = 1
        while bit < size:
            value = value + lax.ppermute(value, axis, [(i, i ^ bit) for i in range(size)])
            bit *= 2
    return value


def exchange(value):
    return lax.all_to_all(value, "tensor", split_axis=0, concat_axis=0, tiled=True)


def reorder(value):
    size = lax.axis_size("tensor")
    return value[jnp.arange(size, dtype=jnp.int32) ^ lax.axis_index("tensor")]


def hand_heads(value):
    size, rows, cols = value.shape
    if size != 4:
        return exchange(reorder(value)).reshape(size * rows, cols)
    place = lax.axis_index("tensor")
    blocks = [value[0]] + [hop(value[r], r) for r in (1, 2, 3)]
    total = jnp.zeros((size * rows, cols), value.dtype)
    for r, block in enumerate(blocks):
        total = lax.dynamic_update_slice_in_dim(total, block, (place ^ r) * rows, 0)
    return total


def return_heads(value):
    if lax.axis_size("tensor") != 4:
        return [reorder(exchange(part)) for part in value]
    place = lax.axis_index("tensor")
    blocks = [
        jnp.stack([lax.dynamic_index_in_dim(part, place ^ r, 0, keepdims=False) for part in value])
        for r in range(4)
    ]
    blocks = [blocks[0]] + [hop(blocks[r], r) for r in (1, 2, 3)]
    return [jnp.stack([block[i] for block in blocks]) for i in range(len(value))]


def core_groups():
    size = lax.axis_size("dp")
    return [list(range(core, size, 2)) for core in (0, 1)]


def core_hop(value):
    size = lax.axis_size("dp")
    return lax.ppermute(value, "dp", [(i, i ^ 1) for i in range(size)])


def gather_lane(shards, axis):
    return lax.all_gather(shards, "dp", axis=axis, tiled=True, axis_index_groups=core_groups())


def gather_plane(lane):
    if lax.axis_size("tensor") == 4:
        own, one, two, low, high = spread_rows(lane)
        lane = two
        mine = jnp.stack([own, one, two, jnp.concatenate([low, high])])
    else:
        mine = reorder(lax.all_gather(lane, "tensor", axis=0, tiled=False))
    return mine, core_hop(mine), lane


def reduce_core(halves):
    mine, other = halves
    return add_low(mine, core_hop(other))


def reduce_plane(total):
    if lax.axis_size("tensor") != 4:
        return lax.psum_scatter(reorder(total), "tensor", scatter_dimension=0, tiled=False)
    half = total.shape[1] // 2
    own, *rest = collect_rows([total[0], total[1], total[2], total[3, :half], total[3, half:]])
    one_low, one_high, two_low, two_high = (x.astype(jnp.float32) for x in rest)
    own = own.astype(jnp.float32)
    return jnp.concatenate(
        [own[:half] + one_low + two_low, own[half:] + one_high + two_high]
    ).astype(total.dtype)


def reduce_lane(value, axis):
    return lax.psum_scatter(
        value, "dp", scatter_dimension=axis, tiled=True, axis_index_groups=core_groups()
    ).astype(jnp.float32)


def contract_first(left, right):
    return low_dot(left, right, ((0,), (0,)))


def contract_last(left, right):
    return low_dot(left, right, ((1,), (1,)))


def split_columns(value):
    size = lax.axis_size("dp")
    rows, cols = value.shape
    return value.reshape(rows, size, cols // size).transpose(1, 0, 2).reshape(size, -1)


def reduce_small(values):
    size = lax.axis_size("dp")
    packed = jnp.concatenate([split_columns(value) for value in values], axis=1)
    length = packed.shape[1]
    rows = -(-length // 1024) * 8
    packed = jnp.pad(packed, ((0, 0), (0, rows * 128 - length))).reshape(size, rows, 128)
    mine = lax.dynamic_index_in_dim(
        sum_all(packed), lax.axis_index("dp"), 0, keepdims=False
    ).reshape(-1)
    result, first = [], 0
    for value in values:
        count = value.shape[0] * value.shape[1] // size
        result.append(mine[first : first + count].reshape(value.shape[0], -1))
        first += count
    return result


def gather_small(values):
    size = lax.axis_size("dp")
    packed = jnp.concatenate([value.reshape(-1) for value in values])
    length = packed.shape[0]
    rows = -(-length // 2048) * 16
    packed = jnp.pad(packed, (0, rows * 128 - length)).reshape(rows, 128)
    every = lax.all_gather(packed, "dp", axis=0, tiled=False).reshape(size, -1)
    result, first = [], 0
    for value in values:
        count = value.size
        block = every[:, first : first + count].reshape(size, value.shape[0], -1)
        result.append(block.transpose(1, 0, 2).reshape(value.shape[0], -1))
        first += count
    return result


def body(
    streams,
    prior,
    seg_ids,
    positions,
    w_qk,
    w_value,
    w_out,
    w_up,
    w_down,
    norm_gain,
    norm_bias,
    mix_in,
    mix_out,
    mix_bias,
    d_streams,
):
    rows_dev = streams.shape[1]
    bf16 = jnp.bfloat16
    gains, shifts, mixin_cols, mixout_all, mixbias_all = gather_small(
        [norm_gain, norm_bias, mix_in.T, mix_out, mix_bias[None]]
    )
    gains, shifts = gains.astype(jnp.float32), shifts.astype(jnp.float32)
    mixout_all, mixbias_all = mixout_all.astype(jnp.float32), mixbias_all.astype(jnp.float32)
    owners = lax.axis_size("dp")
    core = (lax.axis_index("dp") % 2).astype(jnp.int32)[None]
    place = lax.axis_index("tensor").astype(jnp.int32)
    here, still = place[None], jnp.zeros((1,), jnp.int32)
    normed = norm_streams(streams, 3, gains[:3], shifts[:3], core, owners)
    tables = rotary_tables(positions)
    own_tables = [lax.dynamic_slice_in_dim(t, place * rows_dev, rows_dev) for t in tables]
    lanes = [gather_lane(w, 0) for w in (w_value, w_qk[0], w_qk[1])]
    *value_full, mark = gather_plane(after(lanes[0], normed))
    *query_full, mark_two = gather_plane(after(lanes[1], mark))
    *key_full, mark_three = gather_plane(after(lanes[2], mark_two))
    w_out = after(w_out, mark_two, lanes[2])
    out_full = lax.all_gather(w_out, "tensor", axis=0, tiled=False)
    out_full = [lax.all_gather(out_full, "dp", axis=2, tiled=True)]
    w_up = after(w_up, *out_full)
    up_all = lax.all_gather(w_up, "dp", axis=0, tiled=True)
    down_all = lax.all_gather(after(w_down, up_all), "dp", axis=1, tiled=True)

    value = hand_heads(project(normed[2], value_full, still, name="value"))
    query = hand_heads(project(normed[0], query_full, still, own_tables, name="query"))
    key = hand_heads(project(normed[1], key_full, still, own_tables, name="key"))
    heads_shape = value.shape
    attended, logs = attend(query, key, value, positions, seg_ids)
    attended_rows = exchange(attended.reshape(-1, rows_dev, heads_shape[1]))
    attn_result = join(attended_rows, out_full, still, name="attn_out")
    mid, mlp_input = middle(attn_result, streams, gains[3], shifts[3])

    mlp_rows = spread_rows(mlp_input)
    hidden, slopes, parts = [], [], []
    for rows in in_turn(mlp_rows, parts):
        acts, slope = gelu_pair(low_dot(rows, up_all, ((1,), (0,))))
        hidden.append(acts.astype(bf16))
        slopes.append(slope.astype(bf16))
        parts.append(low_dot(hidden[-1], down_all, ((1,), (0,))).astype(bf16))
    parts = collect_rows(parts)
    (
        new_streams,
        grad_prior,
        grad_layer,
        grad_layer_low,
        grad_mix_in,
        grad_mix_out,
        grad_mix_bias,
        gain_four,
        shift_four,
    ) = mixer(
        mid, parts, prior, d_streams, gains[4], shifts[4], mixin_cols, mixout_all, mixbias_all[0]
    )

    grad_rows = spread_rows(grad_layer_low)
    grad_pre, parts = [], []
    for rows, slope in zip(in_turn(grad_rows, parts), slopes):
        grad_hidden = contract_last(rows, down_all)
        grad_pre.append((grad_hidden * slope.astype(jnp.float32)).astype(bf16))
        parts.append(contract_last(grad_pre[-1], up_all).astype(bf16))
    parts = collect_rows(parts)
    grad_w_down = contract_first(jnp.concatenate(hidden), jnp.concatenate(grad_rows)).astype(bf16)
    parts, grad_w_down = lax.optimization_barrier((parts, grad_w_down))
    shard_down = lax.psum_scatter(grad_w_down, "dp", scatter_dimension=1, tiled=True)
    grad_mid, gain_three, shift_three = middle_back(mid, grad_layer, parts, gains[3])

    grad_attended = project(grad_mid, out_full, still, swap=True, name="attn_out_back")
    mlp_rows = after(mlp_rows, grad_attended)
    grad_w_up = contract_first(jnp.concatenate(mlp_rows), jnp.concatenate(grad_pre)).astype(bf16)
    shard_up = lax.psum_scatter(grad_w_up, "dp", scatter_dimension=0, tiled=True)
    grad_attended = after(exchange(grad_attended), grad_w_up)
    grad_query, grad_key, grad_value = attend_back(
        query,
        key,
        value,
        attended,
        grad_attended.reshape(heads_shape),
        logs,
        positions,
        seg_ids,
        *tables,
    )
    rows = return_heads(
        [
            grad.reshape(-1, rows_dev, heads_shape[1])
            for grad in (grad_query, grad_key, grad_value)
        ]
    )
    grad_w_out = head_grad(after(grad_mid, grad_query), attended_rows, here, name="grad_w_out")
    lane_sum_out = lax.psum_scatter(grad_w_out, "dp", scatter_dimension=2, tiled=True)
    totals = []
    back = []
    for part, normed_rows, full in zip(rows, normed, (query_full, key_full, value_full)):
        if back:
            part = after(part, back[-1], totals[-1])
        totals.append(reduce_core(weight_grad(normed_rows, part, still, name="grad_w_in")))
        back.append(join(part, full, still, swap=True, name="attn_in_back"))
    planes = [reduce_plane(total) for total in totals]
    shard_out = reduce_plane(lane_sum_out).astype(jnp.float32)
    back[2] = after(back[2], planes[0], shard_out)
    grad_streams, gain_first, shift_first = streams_back(
        streams, *back, grad_mid, gains[:3], core, owners
    )
    planes[0] = after(planes[0], shard_down, shard_up)
    shard_query, shard_key, shard_value = (reduce_lane(plane, 0) for plane in planes)
    late_gain, late_shift, total_mix_in, total_mix_out, total_mix_bias = reduce_small(
        [
            jnp.concatenate([gain_three, gain_four]),
            jnp.concatenate([shift_three, shift_four]),
            grad_mix_in,
            grad_mix_out,
            grad_mix_bias,
        ]
    )
    early_gain, early_shift = reduce_small([gain_first[:, 0], shift_first[:, 0]])
    return (
        new_streams,
        grad_streams,
        grad_prior,
        jnp.stack([shard_query, shard_key]),
        shard_value,
        shard_out,
        shard_up.astype(jnp.float32),
        shard_down.astype(jnp.float32),
        jnp.concatenate([early_gain, late_gain]),
        jnp.concatenate([early_shift, late_shift]),
        total_mix_in.T,
        total_mix_out,
        total_mix_bias[0],
    )


def solution(mesh):
    in_specs = (
        P(None, ("dp", "tensor"), None),
        P(None, ("dp", "tensor"), None),
        P("dp"),
        P("dp"),
        P(None, "dp", "tensor"),
        P("dp", "tensor"),
        P("tensor", "dp"),
        P("dp", "tensor"),
        P("tensor", "dp"),
        P(None, "dp"),
        P(None, "dp"),
        P("dp", None),
        P(None, "dp"),
        P("dp"),
        P(None, ("dp", "tensor"), None),
    )
    out_specs = (
        P(None, ("dp", "tensor"), None),
        P(None, ("dp", "tensor"), None),
        P(None, ("dp", "tensor"), None),
        P(None, "dp", "tensor"),
        P("dp", "tensor"),
        P("tensor", "dp"),
        P("dp", "tensor"),
        P("tensor", "dp"),
        P(None, "dp"),
        P(None, "dp"),
        P("dp", None),
        P(None, "dp"),
        P("dp"),
    )
    return jax.shard_map(body, mesh=mesh, in_specs=in_specs, out_specs=out_specs, check_vma=False)
```
